256 devices in a mesh: sp: 32 (over z, x), rep: 8 (over y, core).
Axes of the slice: x: 4, y: 4, z: 8, core: 2. Of those that a mesh axis runs over, the one named last changes fastest.
Arguments:
- incoming_embeddings: bfloat16 [8, 64, 256, 512], P('rep', 'sp'), may hold values from -16 to 16
- output_sensitivity: bfloat16 [8, 64, 256, 512], P('rep', 'sp'), may hold values from -6 to 6
- mixing_prenormal_multiplier: float32 [512], replicated, may hold values from 0.5 to 1.5
- triple_mapping_matrix: bfloat16 [512, 1536], replicated, may hold values from -1 to 1
- head_sharpness: float32 [8], replicated, may hold values from 0.5 to 300
- output_mapping_matrix: bfloat16 [512, 512], replicated, may hold values from -0.25 to 0.25
- residual_arm_factors: float32 [2, 512], replicated, may hold values from 0.5 to 1.5
- locality_prenormal_multiplier: float32 [512], replicated, may hold values from 0.5 to 1.5
- separable_kernel_pair: float32 [2, 3, 3, 512], replicated, may hold values from -2 to 2
Outputs:
- grad_input: bfloat16 [8, 64, 256, 512], P('rep', 'sp')
- grad_qkv: float32 [512, 1536], P('rep')
- grad_proj: float32 [512, 512], P('rep')
- grad_conv: float32 [2, 3, 3, 512], replicated
- grad_scale: float32 [2, 512], replicated
The draws below stay inside these ranges and needn't reach their ends.
All inputs are finite; a program needn't handle non-finite values.
Results may differ from the reference program's by a relative error of at most 0.0095.
Values may be sent and summed in bfloat16 or wider, within the bound.
A program may use at most 64 MiB of HBM per device.

```python
import jax
import jax.numpy as jnp
from jax import lax

D = 512
HEADS = 8
HEAD_DIM = 64
WIDTH = 256
HEIGHT = 64
IMAGES = 8


def draw_incoming_embeddings(key, part):
    shape = (IMAGES, HEIGHT, WIDTH, D)
    lean = jax.random.normal(jax.random.fold_in(key, 2), (IMAGES, 1, 1, D), jnp.float32)
    position = jnp.arange(HEIGHT, dtype=jnp.float32) / max(HEIGHT - 1, 1)
    noise = jax.random.normal(jax.random.fold_in(key, 1), shape, jnp.float32)
    rise = 3.0 * position
    values = noise + rise[None, :, None, None] * lean
    return jnp.clip(values, -16.0, 16.0).astype(jnp.bfloat16)


def draw_triple_mapping_matrix(key, part):
    base = jax.random.normal(key, (D, 3 * D), jnp.float32) * D ** (-0.5)
    return jnp.clip(base, -1.0, 1.0).astype(jnp.bfloat16)


def draw_head_sharpness(key, part):
    uniform_draw = jax.random.uniform(key, (HEADS,), jnp.float32)
    temps = 0.5 * jnp.exp(uniform_draw * jnp.log(8.0))
    return temps


def levels(key, dims, shards, least, high):
    gain, own = 1.0, jax.random.fold_in(key, 6)
    for axis_at, blocks in shards:
        heights = jnp.exp(jax.random.uniform(jax.random.fold_in(own, axis_at), (blocks,), jnp.float32, least / len(shards), high / len(shards)))
        gain = gain * jnp.repeat(heights, dims[axis_at] // blocks).reshape([-1 if axis == axis_at else 1 for axis in range(len(dims))])
    return gain


def bell_draw(rng, extent, scale, bound, shards=(), kind=jnp.bfloat16):
    array = scale * jax.random.normal(rng, extent, jnp.float32)
    if shards:
        array = array * levels(rng, extent, shards, -0.22, 0.18)
    return jnp.clip(array, -bound, bound).astype(kind)


def setup_inputs(seed: int = 0) -> dict:
    key_list = jax.random.split(jax.random.key(seed), 10)
    return {
        "incoming_embeddings": draw_incoming_embeddings(jax.random.fold_in(key_list[9], 71), 0),
        "output_sensitivity": bell_draw(key_list[1], (IMAGES, HEIGHT, WIDTH, D), 1.0, 6.0, ((0, 8), (1, 32))),
        "mixing_prenormal_multiplier": jnp.clip(1.0 + 0.1 * jax.random.normal(key_list[2], (D,), jnp.float32), 0.5, 1.5),
        "triple_mapping_matrix": draw_triple_mapping_matrix(jax.random.fold_in(key_list[9], 71), 0),
        "head_sharpness": draw_head_sharpness(jax.random.fold_in(key_list[9], 71), 0),
        "output_mapping_matrix": bell_draw(key_list[5], (D, D), D ** -0.5, 0.25),
        "residual_arm_factors": jnp.clip(1.0 + 0.1 * jax.random.normal(key_list[6], (2, D), jnp.float32), 0.5, 1.5),
        "locality_prenormal_multiplier": jnp.clip(1.0 + 0.1 * jax.random.normal(key_list[7], (D,), jnp.float32), 0.5, 1.5),
        "separable_kernel_pair": bell_draw(key_list[8], (2, 3, 3, D), 9 ** -0.5, 2.0, (), jnp.float32),
    }


EPS = 1e-06

def conv_valid(padded, kernel):
    row_count = padded.shape[0] - 2
    col_count = padded.shape[1] - 2
    total = jnp.zeros((row_count, col_count, padded.shape[2]), jnp.float32)
    for offset_row in range(3):
        for offset_col in range(3):
            total = total + padded[offset_row:offset_row + row_count, offset_col:offset_col + col_count] * kernel[offset_row, offset_col]
    return total

def gelu_grad(values):
    cumul = 0.5 * (1.0 + lax.erf(values * 0.7071067811865476))
    density = jnp.exp(-0.5 * values * values) * 0.3989422804014327
    return cumul + values * density

def norm_rows(values, gain_vec):
    floated = values.astype(jnp.float32)
    centre = lax.optimization_barrier(jnp.mean(floated, -1, keepdims=True))
    centred = floated - centre
    variance = lax.optimization_barrier(jnp.mean(centred * centred, -1, keepdims=True))
    inverse = lax.rsqrt(variance + EPS)
    normed = centred * inverse
    return (normed * gain_vec, normed, inverse)

def norm_back(upstream, gain_vec, normed, inverse):
    scaled = upstream * gain_vec
    return inverse * (scaled - lax.optimization_barrier(jnp.mean(scaled, -1, keepdims=True)) - normed * lax.optimization_barrier(jnp.mean(scaled * normed, -1, keepdims=True)))

def single_slide_evaluate(slide_embeddings, slide_sensitivities, mixing_prenormal_multiplier, triple_mapping_matrix, head_sharpness, output_mapping_matrix, residual_arm_factors, locality_prenormal_multiplier, separable_kernel_pair):
    high = lax.Precision.HIGHEST
    token_count = HEIGHT * WIDTH
    flat_rows = slide_embeddings.reshape(token_count, D)
    act_one, normed_one, inverse_one = norm_rows(flat_rows, mixing_prenormal_multiplier)
    act_one = act_one.astype(jnp.bfloat16)
    mixed_rows = jnp.dot(act_one, triple_mapping_matrix, preferred_element_type=jnp.float32).astype(jnp.bfloat16)
    query_f = mixed_rows[:, :D].astype(jnp.float32).reshape(token_count, HEADS, HEAD_DIM)
    key_f = mixed_rows[:, D:2 * D].astype(jnp.float32).reshape(token_count, HEADS, HEAD_DIM)
    value_f = mixed_rows[:, 2 * D:].astype(jnp.float32).reshape(token_count, HEADS, HEAD_DIM)
    covariance_accumulated = jnp.einsum('mhc,mhe->hce', query_f, key_f, precision=high)
    query_norm = jnp.sqrt(lax.optimization_barrier(jnp.sum(query_f * query_f, 0)) + EPS)
    key_norm = jnp.sqrt(lax.optimization_barrier(jnp.sum(key_f * key_f, 0)) + EPS)
    softmax_divisor = query_norm[:, :, None] * key_norm[:, None, :]
    feature_affinity_logits = head_sharpness[:, None, None] * covariance_accumulated / softmax_divisor
    shifted = feature_affinity_logits - lax.optimization_barrier(jnp.max(feature_affinity_logits, -1, keepdims=True))
    exponent = jnp.exp(shifted)
    attn_prob = exponent / lax.optimization_barrier(jnp.sum(exponent, -1, keepdims=True))
    prob_low = attn_prob.astype(jnp.bfloat16)
    attended = jnp.einsum('hce,mhe->mhc', prob_low.astype(jnp.float32), value_f, precision=high)
    attended = attended.reshape(token_count, D).astype(jnp.bfloat16)
    projected = jnp.dot(attended, output_mapping_matrix, preferred_element_type=jnp.float32)
    residual = (flat_rows.astype(jnp.float32) + residual_arm_factors[0] * projected).astype(jnp.bfloat16)
    act_two, normed_two, inverse_two = norm_rows(residual, locality_prenormal_multiplier)
    act_two = act_two.astype(jnp.bfloat16)
    upstream = slide_sensitivities.astype(jnp.float32)
    padded_in = jnp.pad(act_two.reshape(HEIGHT, WIDTH, D).astype(jnp.float32), ((1, 1), (1, 1), (0, 0)))
    h_one, back_one = jax.vjp(conv_valid, padded_in, separable_kernel_pair[0])
    hidden = jax.nn.gelu(h_one, approximate=False).astype(jnp.bfloat16)
    padded_hid = jnp.pad(hidden.astype(jnp.float32), ((1, 1), (1, 1), (0, 0)))
    spatial, back_two = jax.vjp(conv_valid, padded_hid, separable_kernel_pair[1])
    d_pad_hid, grad_w_two = back_two(residual_arm_factors[1] * upstream)
    d_h_one = d_pad_hid[1:-1, 1:-1] * gelu_grad(h_one)
    d_pad_in, grad_w_one = back_one(d_h_one)
    d_act_two = d_pad_in[1:-1, 1:-1].reshape(token_count, D)
    up_flat = upstream.reshape(token_count, D)
    scale_two = lax.optimization_barrier(jnp.sum(spatial.reshape(token_count, D) * up_flat, 0))
    d_residual = up_flat + norm_back(d_act_two, locality_prenormal_multiplier, normed_two, inverse_two)
    scale_one = lax.optimization_barrier(jnp.sum(projected * d_residual, 0))
    d_proj = (residual_arm_factors[0] * d_residual).astype(jnp.bfloat16)
    grad_proj = jnp.dot(attended.T, d_proj, preferred_element_type=jnp.float32)
    d_attended = jnp.dot(d_proj, output_mapping_matrix.T, preferred_element_type=jnp.float32).astype(jnp.bfloat16)
    d_att_f = d_attended.astype(jnp.float32).reshape(token_count, HEADS, HEAD_DIM)
    prob_grad = jnp.einsum('mhc,mhe->hce', d_att_f, value_f, precision=high)
    d_value = jnp.einsum('hce,mhc->mhe', prob_low.astype(jnp.float32), d_att_f, precision=high)
    logit_sensitivity = attn_prob * (prob_grad - lax.optimization_barrier(jnp.sum(attn_prob * prob_grad, -1, keepdims=True)))
    covariance_sensitivity = (logit_sensitivity * head_sharpness[:, None, None] / softmax_divisor).astype(jnp.bfloat16).astype(jnp.float32)
    weighted = logit_sensitivity * feature_affinity_logits
    d_qsq = -lax.optimization_barrier(jnp.sum(weighted, -1)) / (2.0 * query_norm * query_norm)
    d_ksq = -lax.optimization_barrier(jnp.sum(weighted, 1)) / (2.0 * key_norm * key_norm)
    d_query = jnp.einsum('hce,mhe->mhc', covariance_sensitivity, key_f, precision=high) + 2.0 * d_qsq * query_f
    d_key = jnp.einsum('hce,mhc->mhe', covariance_sensitivity, query_f, precision=high) + 2.0 * d_ksq * key_f
    d_mixed = jnp.concatenate([d_query.reshape(token_count, D), d_key.reshape(token_count, D), d_value.reshape(token_count, D)], -1).astype(jnp.bfloat16)
    grad_qkv = jnp.dot(act_one.T, d_mixed, preferred_element_type=jnp.float32)
    d_act_one = jnp.dot(d_mixed, triple_mapping_matrix.T, preferred_element_type=jnp.float32)
    d_tokens = (d_residual + norm_back(d_act_one, mixing_prenormal_multiplier, normed_one, inverse_one)).astype(jnp.bfloat16)
    return (d_tokens.reshape(HEIGHT, WIDTH, D), grad_qkv, grad_proj, jnp.stack([grad_w_one, grad_w_two]), jnp.stack([scale_one, scale_two]))

def reference(incoming_embeddings, output_sensitivity, mixing_prenormal_multiplier, triple_mapping_matrix, head_sharpness, output_mapping_matrix, residual_arm_factors, locality_prenormal_multiplier, separable_kernel_pair):

    def one_image(zipped_entries):
        return single_slide_evaluate(zipped_entries[0], zipped_entries[1], mixing_prenormal_multiplier, triple_mapping_matrix, head_sharpness, output_mapping_matrix, residual_arm_factors, locality_prenormal_multiplier, separable_kernel_pair)
    results = lax.map(one_image, (incoming_embeddings, output_sensitivity))
    return (results[0], lax.optimization_barrier(jnp.sum(results[1], 0)), lax.optimization_barrier(jnp.sum(results[2], 0)), lax.optimization_barrier(jnp.sum(results[3], 0)), lax.optimization_barrier(jnp.sum(results[4], 0)))
```

```python
import functools

import jax
import jax.numpy as jnp
from jax import lax
from jax.experimental import pallas as pl
from jax.experimental.pallas import tpu as pltpu
from jax.sharding import PartitionSpec as P

D = 512
HEADS = 8
HEAD_DIM = 64
WIDTH = 256
EPS = 1e-06
F32 = jnp.float32
BF16 = jnp.bfloat16
TOK = 512
PAIRS = 4
VMEM = pltpu.VMEM
MESH_ID = pl.DeviceIdType.MESH
LIMIT = 60 * 1024 * 1024


def dot(a, b, ca, cb):
    return lax.dot_general(a, b, (((ca,), (cb,)), ((), ())), preferred_element_type=F32)


def ds(start, size, multiple=None):
    return pl.ds(pl.multiple_of(start, multiple or size), size)


def norm_parts(u):
    centre = jnp.mean(u, -1, keepdims=True)
    centred = u - centre
    inverse = lax.rsqrt(jnp.mean(centred * centred, -1, keepdims=True) + EPS)
    return centred * inverse, inverse


def norm_back(upstream, gain, normed, inverse):
    scaled = upstream * gain
    return inverse * (
        scaled
        - jnp.mean(scaled, -1, keepdims=True)
        - normed * jnp.mean(scaled * normed, -1, keepdims=True)
    )


def lane_low():
    return lax.broadcasted_iota(jnp.int32, (HEAD_DIM, 128), 1) < HEAD_DIM


def eye_pair():
    lane = lax.broadcasted_iota(jnp.int32, (HEAD_DIM, 128), 1)
    row = lax.broadcasted_iota(jnp.int32, (HEAD_DIM, 128), 0)
    return (lane == row) | (lane == row + HEAD_DIM)


def half_sum(v, low):
    left = jnp.sum(jnp.where(low, v, 0.0), -1, keepdims=True)
    right = jnp.sum(jnp.where(low, 0.0, v), -1, keepdims=True)
    return jnp.where(low, left, right)


def half_max(v, low):
    left = jnp.max(jnp.where(low, v, -jnp.inf), -1, keepdims=True)
    right = jnp.max(jnp.where(low, -jnp.inf, v), -1, keepdims=True)
    return jnp.where(low, left, right)


def pack_pair(full, low):
    return jnp.where(low, full[:HEAD_DIM], full[HEAD_DIM:])


def block_diag(packed, low):
    return jnp.concatenate(
        [jnp.where(low, packed, 0.0), jnp.where(low, 0.0, packed)], axis=0
    ).astype(BF16)


def pair_attention(p, gram_ref, sq_ref, sharp_ref, low, eye):
    gram = gram_ref[8 * p : 8 * p + 8].reshape(HEAD_DIM, 128)
    query_sq = half_sum(jnp.where(eye, sq_ref[p : p + 1, :], 0.0), low)
    query_norm = jnp.sqrt(query_sq + EPS)
    key_norm = jnp.sqrt(sq_ref[PAIRS + p : PAIRS + p + 1, :] + EPS)
    divisor = query_norm * key_norm
    sharp = jnp.where(low, sharp_ref[2 * p], sharp_ref[2 * p + 1])
    scores = sharp * gram / divisor
    exponent = jnp.exp(scores - half_max(scores, low))
    prob = exponent / half_sum(exponent, low)
    return prob, scores, divisor, sharp, query_norm, key_norm


def first_part(x_ref, gain_ref, w_ref, act_ref, mixed_ref, msg_ref):
    gain = gain_ref[...]

    def rows(i, _):
        at = ds(i * 32, 32)
        normed, _ = norm_parts(x_ref[at, :].astype(F32))
        act_ref[at, :] = (normed * gain).astype(BF16)
        return 0

    lax.fori_loop(0, TOK // 32, rows, 0)

    def mix(i, _):
        at = ds(i * 256, 256)
        mixed_ref[at, :] = dot(act_ref[at, :], w_ref[...], 1, 0).astype(BF16)
        return 0

    lax.fori_loop(0, TOK // 256, mix, 0)
    low = lane_low()
    sums = []
    for p in range(2 * PAIRS):
        sq = jnp.zeros((8, 128), F32)
        for i in range(0, TOK, 64):
            part = mixed_ref[i : i + 64, 128 * p : 128 * p + 128].astype(F32)
            sq = sq + (part * part).reshape(8, 8, 128).sum(0)
        sums.append(sq.sum(0, keepdims=True))
    sq = jnp.concatenate(sums, axis=0)
    for p in range(PAIRS):
        query = mixed_ref[:, 128 * p : 128 * p + 128]
        key = mixed_ref[:, D + 128 * p : D + 128 * p + 128]
        packed = pack_pair(dot(query, key, 0, 0), low)
        for b in range(8):
            msg_ref[8 * p + b, 0:8, :] = packed[8 * b : 8 * b + 8]
    for j in range(32):
        msg_ref[j, 8:16, :] = sq


def remote(src, dst, send, recv, **axes):
    return pltpu.make_async_remote_copy(
        src_ref=src, dst_ref=dst, send_sem=send, recv_sem=recv, device_id=axes, device_id_type=MESH_ID
    )


def greet_strips(n, me, barrier):
    def greet(k, _):
        pl.semaphore_signal(
            barrier, inc=1, device_id={"sp": lax.rem(me + k, n)}, device_id_type=MESH_ID
        )
        return 0

    lax.fori_loop(1, n, greet, 0)


def strip_sum(n, me, msg_ref, total_ref, got, mine, sems, rows, between):
    def first(k):
        j = lax.rem(me + k, n)
        return remote(msg_ref.at[j], got.at[k], sems[0].at[k], sems[1].at[k], sp=j)

    def second(k):
        j = lax.rem(me + k, n)
        return remote(mine, total_ref.at[me], sems[2].at[k], sems[3].at[k], sp=j)

    def start(copy):
        def go(k, _):
            copy(k).start()
            return 0

        lax.fori_loop(1, n, go, 0)

    start(first)
    between()

    def add(k, total):
        first(k).wait_recv()
        return total + got[k]

    total = lax.fori_loop(1, n, add, msg_ref[me])
    mine[...] = total[:rows]
    start(second)
    total_ref[me] = total[:rows]

    def finish(k, _):
        second(k).wait_recv()
        second(k).wait_send()
        first(k).wait_send()
        return 0

    return total, lambda: lax.fori_loop(1, n, finish, 0)


def gram_exchange(
    n, msg_ref, x_ref, up_ref, gram_ref, sq_ref, xe_ref, ue_ref, got, mine, s0, s1, s2, s3, hs, hr
):
    me = lax.axis_index("sp")
    below, above = lax.rem(me + 1, n), lax.rem(me + n - 1, n)
    barrier = pltpu.get_barrier_semaphore()
    greet_strips(n, me, barrier)
    pl.semaphore_wait(barrier, n - 1)
    halos = []
    for at, (src, dst) in enumerate(((x_ref, xe_ref), (up_ref, ue_ref))):
        halos.append(remote(src, dst.at[pl.ds(0, TOK)], hs.at[2 * at], hr.at[2 * at], sp=below))
        halos.append(
            remote(src, dst.at[pl.ds(2 * TOK, TOK)], hs.at[2 * at + 1], hr.at[2 * at + 1], sp=above)
        )

    def between():
        for copy in halos:
            copy.start()
        xe_ref[TOK : 2 * TOK, :] = x_ref[...]
        ue_ref[TOK : 2 * TOK, :] = up_ref[...]

    total, finish = strip_sum(n, me, msg_ref, gram_ref, got, mine, (s0, s1, s2, s3), 8, between)
    sq_ref[...] = total[8:]
    finish()
    for copy in halos:
        copy.wait()


def prob_exchange(n, msg_ref, prob_ref, small_ref, got, mine, s0, s1, s2, s3):
    me = lax.axis_index("sp")
    barrier = pltpu.get_barrier_semaphore()
    greet_strips(n, me, barrier)
    pl.semaphore_wait(barrier, n - 1)
    total, finish = strip_sum(
        n, me, msg_ref, prob_ref, got, mine, (s0, s1, s2, s3), 8, lambda: None
    )
    small_ref[...] = total[8:]
    finish()


def middle_part(
    n,
    sharp_ref,
    gram_ref,
    sq_ref,
    xe_ref,
    ue_ref,
    mixed_ref,
    w_ref,
    wo_ref,
    gain1_ref,
    gain2_ref,
    factor_ref,
    kern_ref,
    att_ref,
    dproj_ref,
    dval_ref,
    dres_ref,
    msg_ref,
    bd_s,
    ve_s,
    act_s,
    up_s,
    dh_s,
    hid_s,
    attrow_s,
    projrow_s,
    proj_s,
    normed_s,
    inv_s,
    dact_s,
    acc_s,
    datt_s,
):
    me = lax.axis_index("sp")
    first, last = me == 0, me == n - 1
    low, eye = lane_low(), eye_pair()
    for p in range(PAIRS):
        prob = pair_attention(p, gram_ref, sq_ref, sharp_ref, low, eye)[0]
        bd_s[p] = block_diag(prob, low)
    for ref, count in ((act_s, 6), (up_s, 6), (dh_s, 4), (hid_s, 4)):
        for r in range(count):
            ref[r, 0:8, :] = jnp.zeros((8, D), F32)
            ref[r, 264:272, :] = jnp.zeros((8, D), F32)
    acc_s[...] = jnp.zeros_like(acc_s)
    gain1, gain2 = gain1_ref[...], gain2_ref[...]
    factor0, factor1 = factor_ref[0:1, :], factor_ref[1:2, :]

    def outside(row):
        return ((row < 2) & first) | ((row > 3) & last)

    ve_s[TOK : 2 * TOK, :] = mixed_ref[:, 2 * D :]

    def halo_values(i, _):
        row = i + 2 * (i >= 2).astype(jnp.int32)

        def rows(c, _):
            at = ds(row * WIDTH + c * 32, 32)
            normed, _ = norm_parts(xe_ref[at, :].astype(F32))
            attrow_s[ds(c * 32, 32), :] = (normed * gain1).astype(BF16)
            return 0

        lax.fori_loop(0, WIDTH // 32, rows, 0)
        ve_s[ds(row * WIDTH, WIDTH), :] = dot(attrow_s[...], w_ref[:, 2 * D :], 1, 0).astype(BF16)
        return 0

    lax.fori_loop(0, 4, halo_values, 0)

    def forward_row(row, _):
        at_row = ds(row * WIDTH, WIDTH)
        for p in range(PAIRS):
            cols = slice(128 * p, 128 * p + 128)
            attrow_s[:, cols] = dot(ve_s[at_row, cols], bd_s[p], 1, 1).astype(BF16)
        projrow_s[...] = dot(attrow_s[...], wo_ref[...], 1, 0)
        keep = jnp.logical_not(outside(row))

        def rows(c, _):
            here = ds(c * 32, 32)
            u = xe_ref[ds(row * WIDTH + c * 32, 32), :].astype(F32) + factor0 * projrow_s[here, :]
            normed, inverse = norm_parts(u.astype(BF16).astype(F32))
            act = (normed * gain2).astype(BF16).astype(F32)
            act_s[row, ds(8 + c * 32, 32, 8), :] = jnp.where(keep, act, 0.0)

            @pl.when((row == 2) | (row == 3))
            def _():
                there = ds((row - 2) * WIDTH + c * 32, 32)
                att_ref[there, :] = attrow_s[here, :]
                proj_s[there, :] = projrow_s[here, :]
                normed_s[there, :] = normed
                inv_s[there, :] = jnp.broadcast_to(inverse, (32, 128))

            return 0

        lax.fori_loop(0, WIDTH // 32, rows, 0)
        return 0

    lax.fori_loop(0, 6, forward_row, 0)

    def upstream_rows(i, _):
        row, c = i // 4, lax.rem(i, 4)
        up = ue_ref[ds(row * WIDTH + c * 64, 64), :].astype(F32)
        up_s[row, ds(8 + c * 64, 64, 8), :] = jnp.where(outside(row), 0.0, up)
        return 0

    lax.fori_loop(0, 24, upstream_rows, 0)

    def taps(which, lanes, i, j):
        at = 9 * which + 3 * i + j
        return kern_ref[at : at + 1, lanes]

    def hidden_rows(idx, _):
        hrow, rest = idx // 16, lax.rem(idx, 16)
        lanes, c = ds((rest // 4) * 128, 128), lax.rem(rest, 4)
        win = ds(c * 64, 80, 8)
        near = [act_s[hrow + i, win, lanes] for i in range(3)]
        sums = []
        for j in range(3):
            sums.append(sum(taps(0, lanes, i, j) * near[i] for i in range(3)))
        h = (
            pltpu.roll(sums[0], 1, 0)[8:72]
            + sums[1][8:72]
            + pltpu.roll(sums[2], 79, 0)[8:72]
        )
        near = [up_s[hrow + 2 - i, win, lanes] for i in range(3)]
        sums = []
        scale = factor_ref[1:2, lanes]
        for j in range(3):
            sums.append(sum((taps(1, lanes, i, j) * scale) * near[i] for i in range(3)))
        d_hidden = (
            pltpu.roll(sums[0], 79, 0)[8:72]
            + sums[1][8:72]
            + pltpu.roll(sums[2], 1, 0)[8:72]
        )
        cumul = 0.5 * (1.0 + lax.erf(h * 0.7071067811865476))
        density = jnp.exp(-0.5 * h * h) * 0.3989422804014327
        there = ds(8 + c * 64, 64, 8)
        hid_s[hrow, there, lanes] = (h * cumul).astype(BF16).astype(F32)
        d_h = d_hidden * (cumul + h * density)
        dh_s[hrow, there, lanes] = jnp.where(outside(hrow + 1), 0.0, d_h)
        return 0

    lax.fori_loop(0, 64, hidden_rows, 0)

    def fold(v):
        return v.reshape(8, 8, 128).sum(0)

    def back_rows(idx, _):
        r, rest = idx // 16, lax.rem(idx, 16)
        lanes, c = ds((rest // 4) * 128, 128), lax.rem(rest, 4)
        win, mid = ds(c * 64, 80, 8), ds(8 + c * 64, 64, 8)
        near = [dh_s[r + 2 - i, win, lanes] for i in range(3)]
        sums = []
        for j in range(3):
            sums.append(sum(taps(0, lanes, i, j) * near[i] for i in range(3)))
        dact_s[ds(r * WIDTH + c * 64, 64), lanes] = (
            pltpu.roll(sums[0], 79, 0)[8:72]
            + sums[1][8:72]
            + pltpu.roll(sums[2], 1, 0)[8:72]
        )
        own = near[1]
        moved = [pltpu.roll(own, 79, 0)[8:72], own[8:72], pltpu.roll(own, 1, 0)[8:72]]
        for i in range(3):
            act = act_s[r + 1 + i, mid, lanes]
            for j in range(3):
                acc_s[3 * i + j, :, lanes] += fold(moved[j] * act)
        own = hid_s[r + 1, win, lanes]
        moved = [pltpu.roll(own, 1, 0)[8:72], own[8:72], pltpu.roll(own, 79, 0)[8:72]]
        for i in range(3):
            up = up_s[r + 3 - i, mid, lanes]
            for j in range(3):
                acc_s[9 + 3 * i + j, :, lanes] += fold(moved[j] * up)
        return 0

    lax.fori_loop(0, 32, back_rows, 0)

    def residual_rows(i, scale):
        row, c = i // 8, lax.rem(i, 8)
        at = ds(i * 32, 32)
        lnb = norm_back(dact_s[at, :], gain2, normed_s[at, :], inv_s[at, 0:1])
        d_res = up_s[row + 2, ds(8 + c * 32, 32, 8), :] + lnb
        dres_ref[at, :] = d_res
        dproj_ref[at, :] = (factor0 * d_res).astype(BF16)
        return scale + (proj_s[at, :] * d_res).reshape(4, 8, D).sum(0)

    scale_one = lax.fori_loop(0, TOK // 32, residual_rows, jnp.zeros((8, D), F32))
    lines = [acc_s[m].sum(0, keepdims=True) for m in range(18)]
    scale_two = sum(lines[9 + m] * kern_ref[9 + m : 10 + m, :] for m in range(9))
    lines = lines[:9] + [line * factor1 for line in lines[9:]]
    lines += [scale_one.sum(0, keepdims=True), scale_two]
    for j in range(32):
        msg_ref[j, 8:16, :] = jnp.zeros((8, 128), F32)
    for at in range(80):
        v, b = at // 4, at % 4
        msg_ref[at // 3, 8 + at % 3 : 9 + at % 3, :] = lines[v][:, 128 * b : 128 * b + 128]

    def attended_rows(i, _):
        at = ds(i * 256, 256)
        datt_s[at, :] = dot(dproj_ref[at, :], wo_ref[...], 1, 1).astype(BF16)
        for p in range(PAIRS):
            cols = slice(128 * p, 128 * p + 128)
            dval_ref[at, cols] = dot(datt_s[at, cols], bd_s[p], 1, 0).astype(BF16)
        return 0

    lax.fori_loop(0, 2, attended_rows, 0)
    for p in range(PAIRS):
        cols = slice(128 * p, 128 * p + 128)
        packed = pack_pair(dot(datt_s[:, cols], ve_s[TOK : 2 * TOK, cols], 0, 0), low)
        for b in range(8):
            msg_ref[8 * p + b, 0:8, :] = packed[8 * b : 8 * b + 8]


def last_part(
    sharp_ref,
    gram_ref,
    sq_ref,
    pg_ref,
    x_ref,
    act_ref,
    mixed_ref,
    w_ref,
    gain1_ref,
    att_ref,
    dproj_ref,
    dval_ref,
    dres_ref,
    out_ref,
    grads_ref,
    dmix_s,
    dact_s,
):
    low, eye = lane_low(), eye_pair()
    for p in range(PAIRS):
        prob, scores, divisor, sharp, query_norm, key_norm = pair_attention(
            p, gram_ref, sq_ref, sharp_ref, low, eye
        )
        pg = pg_ref[8 * p : 8 * p + 8].reshape(HEAD_DIM, 128)
        logit = prob * (pg - half_sum(prob * pg, low))
        bd = block_diag(logit * sharp / divisor, low)
        weighted = logit * scores
        d_qsq = -half_sum(weighted, low) / (2.0 * query_norm * query_norm)
        d_qsq = jnp.sum(jnp.where(eye, d_qsq, 0.0), 0, keepdims=True)
        d_ksq = -jnp.sum(weighted, 0, keepdims=True) / (2.0 * key_norm * key_norm)
        qc = slice(128 * p, 128 * p + 128)
        kc = slice(D + 128 * p, D + 128 * p + 128)
        for i in range(0, TOK, 256):
            at = slice(i, i + 256)
            query, key = mixed_ref[at, qc], mixed_ref[at, kc]
            dmix_s[at, qc] = (dot(key, bd, 1, 1) + 2.0 * d_qsq * query.astype(F32)).astype(BF16)
            dmix_s[at, kc] = (dot(query, bd, 1, 0) + 2.0 * d_ksq * key.astype(F32)).astype(BF16)
    dmix_s[:, 2 * D :] = dval_ref[...]

    def inputs(i, _):
        at = ds(i * 256, 256)
        dact_s[at, :] = dot(dmix_s[at, :], w_ref[...], 1, 1)
        return 0

    lax.fori_loop(0, 2, inputs, 0)
    gain1 = gain1_ref[...]

    def rows(i, _):
        at = ds(i * 32, 32)
        normed, inverse = norm_parts(x_ref[at, :].astype(F32))
        lnb = norm_back(dact_s[at, :], gain1, normed, inverse)
        out_ref[at, :] = (dres_ref[at, :] + lnb).astype(BF16)
        return 0

    lax.fori_loop(0, TOK // 32, rows, 0)
    for half in range(2):
        for block in range(4):
            cols = slice(512 * block, 512 * block + 512)
            left = act_ref if block < 3 else att_ref
            right = dmix_s[:, cols] if block < 3 else dproj_ref[...]
            g = dot(left[:, 256 * half : 256 * half + 256], right, 0, 0).astype(BF16)
            for r in range(4):
                rep = 4 * half + r
                grads_ref[rep % 2, rep // 2, :, cols] = g[64 * r : 64 * r + 64]


def grad_exchange(
    n,
    grads_ref,
    small_ref,
    gq_ref,
    gp_ref,
    conv_ref,
    scale_ref,
    rb1,
    sb2,
    rb2,
    acc,
    sb3,
    rb3,
    fin,
    rb4,
    srb,
    sfin,
    sout,
    a0,
    a1,
    b0,
    b1,
    c0,
    c1,
    d0,
    d1,
    e0,
    e1,
    f0,
    f1,
):
    me = lax.axis_index("sp")
    rep = lax.axis_index("rep")
    reps = 8
    y, core = rep // 2, lax.rem(rep, 2)
    barrier = pltpu.get_barrier_semaphore()
    greet_strips(n, me, barrier)
    for k in range(1, reps):
        pl.semaphore_signal(
            barrier, inc=1, device_id={"rep": lax.rem(rep + k, reps)}, device_id_type=MESH_ID
        )
    pl.semaphore_wait(barrier, n - 1 + reps - 1)
    partner = 2 * y + 1 - core
    pair = []
    for k in range(4):
        there = lax.rem(y + 1 + k, 4)
        pair.append(
            remote(grads_ref.at[1 - core, there], rb1.at[k], a0.at[k], a1.at[k], rep=partner)
        )
    for copy in pair:
        copy.start()
    smalls = []
    for k in range(1, reps):
        smalls.append(
            remote(small_ref, srb.at[rep], e0.at[k], e1.at[k], rep=lax.rem(rep + k, reps))
        )
    for copy in smalls:
        copy.start()
    srb[rep] = small_ref[...]
    columns = []
    for k in range(3):
        there = lax.rem(y + 1 + k, 4)
        pair[k].wait_recv()

        def add(i, _, k=k, there=there):
            at = ds(i * 16, 16)
            sb2[k, at, :] = (
                grads_ref[core, there, at, :].astype(F32) + rb1[k, at, :].astype(F32)
            ).astype(BF16)
            return 0

        lax.fori_loop(0, 4, add, 0)
        copy = remote(sb2.at[k], rb2.at[k], b0.at[k], b1.at[k], rep=2 * there + core)
        copy.start()
        columns.append(copy)
    pair[3].wait_recv()

    def own(i, _):
        at = ds(i * 16, 16)
        acc[at, :] = grads_ref[core, y, at, :].astype(F32) + rb1[3, at, :].astype(F32)
        return 0

    lax.fori_loop(0, 4, own, 0)
    for copy in columns:
        copy.wait_recv()
    for j in range(n):
        rows, cols = slice(32 * (j // 16), 32 * (j // 16) + 32), slice(128 * (j % 16), 128 * (j % 16) + 128)
        total = acc[rows, cols]
        for k in range(3):
            total = total + rb2[k, rows, cols].astype(F32)
        sb3[j] = total.astype(BF16)

    def third(k):
        j = lax.rem(me + k, n)
        return remote(sb3.at[j], rb3.at[k], c0.at[k], c1.at[k], sp=j)

    def fourth(k):
        return remote(fin, rb4.at[me], d0.at[k], d1.at[k], sp=lax.rem(me + k, n))

    def fifth(k):
        return remote(sfin, sout.at[me], f0.at[k], f1.at[k], sp=lax.rem(me + k, n))

    def start_third(k, _):
        third(k).start()
        return 0

    lax.fori_loop(1, n, start_third, 0)
    for copy in smalls:
        copy.wait_recv()
    total = srb[0]
    for k in range(1, reps):
        total = total + srb[k]
    sfin[...] = total
    sout[me] = total

    def start_fifth(k, _):
        fifth(k).start()
        return 0

    lax.fori_loop(1, n, start_fifth, 0)

    def add_third(k, total):
        third(k).wait_recv()
        return total + rb3[k].astype(F32)

    total = lax.fori_loop(1, n, add_third, sb3[me].astype(F32)).astype(BF16)
    fin[...] = total
    rb4[me] = total

    def start_fourth(k, _):
        fourth(k).start()
        return 0

    lax.fori_loop(1, n, start_fourth, 0)

    def finish(k, _):
        fourth(k).wait_recv()
        fifth(k).wait_recv()
        fourth(k).wait_send()
        fifth(k).wait_send()
        third(k).wait_send()
        return 0

    lax.fori_loop(1, n, finish, 0)
    for j in range(n):
        rows, at = slice(32 * (j // 16), 32 * (j // 16) + 32), 128 * (j % 16)
        if at < 3 * D:
            gq_ref[rows, at : at + 128] = rb4[j].astype(F32)
        else:
            gp_ref[rows, at - 3 * D : at - 3 * D + 128] = rb4[j].astype(F32)
    for at in range(80):
        v, b = at // 4, at % 4
        line = sout[at // 3, at % 3 : at % 3 + 1, :]
        if v < 18:
            conv_ref[v : v + 1, 128 * b : 128 * b + 128] = line
        else:
            scale_ref[v - 18 : v - 17, 128 * b : 128 * b + 128] = line
    for copy in pair + smalls + columns:
        copy.wait_send()


def call(body, name, outs, scratch, args, smem=0, collective=None):
    params = dict(vmem_limit_bytes=LIMIT)
    if collective is not None:
        params.update(collective_id=collective, has_side_effects=True)
    specs = [pl.BlockSpec(memory_space=pltpu.SMEM)] * smem
    specs += [pl.BlockSpec(memory_space=VMEM)] * (len(args) - smem)
    return pl.pallas_call(
        body,
        name=name,
        out_shape=[jax.ShapeDtypeStruct(s, t) for s, t in outs],
        in_specs=specs,
        out_specs=[pl.BlockSpec(memory_space=VMEM)] * len(outs),
        scratch_shapes=scratch,
        compiler_params=pltpu.CompilerParams(**params),
    )(*args)


def dma(*counts):
    return [pltpu.SemaphoreType.DMA((c,)) for c in counts]


def shards(n, x, up, gain1, w, sharp, wo, factors, gain2, kernels):
    x = x.reshape(TOK, D)
    up = up.reshape(TOK, D)
    gain1, gain2 = gain1.reshape(1, D), gain2.reshape(1, D)
    kern = kernels.reshape(18, D)
    act, mixed, msg = call(
        first_part,
        "first_part",
        [((TOK, D), BF16), ((TOK, 3 * D), BF16), ((n, 16, 128), F32)],
        [],
        (x, gain1, w),
    )
    gram, sq, xe, ue = call(
        functools.partial(gram_exchange, n),
        "gram_exchange",
        [((n, 8, 128), F32), ((8, 128), F32), ((3 * TOK, D), BF16), ((3 * TOK, D), BF16)],
        [VMEM((n, 16, 128), F32), VMEM((8, 128), F32)] + dma(n, n, n, n, 4, 4),
        (msg, x, up),
        collective=0,
    )
    att, dproj, dval, dres, msg = call(
        functools.partial(middle_part, n),
        "middle_part",
        [((TOK, D), BF16)] * 3 + [((TOK, D), F32), ((n, 16, 128), F32)],
        [
            VMEM((PAIRS, 128, 128), BF16),
            VMEM((3 * TOK, D), BF16),
            VMEM((6, 272, D), F32),
            VMEM((6, 272, D), F32),
            VMEM((4, 272, D), F32),
            VMEM((4, 272, D), F32),
            VMEM((WIDTH, D), BF16),
            VMEM((WIDTH, D), F32),
            VMEM((TOK, D), F32),
            VMEM((TOK, D), F32),
            VMEM((TOK, 128), F32),
            VMEM((TOK, D), F32),
            VMEM((18, 8, D), F32),
            VMEM((TOK, D), BF16),
        ],
        (sharp, gram, sq, xe, ue, mixed, w, wo, gain1, gain2, factors, kern),
        smem=1,
    )
    pg, small = call(
        functools.partial(prob_exchange, n),
        "prob_exchange",
        [((n, 8, 128), F32), ((8, 128), F32)],
        [VMEM((n, 16, 128), F32), VMEM((8, 128), F32)] + dma(n, n, n, n),
        (msg,),
        collective=1,
    )
    out, grads = call(
        last_part,
        "last_part",
        [((TOK, D), BF16), ((2, 4, 64, 2048), BF16)],
        [VMEM((TOK, 3 * D), BF16), VMEM((TOK, D), F32)],
        (sharp, gram, sq, pg, x, act, mixed, w, gain1, att, dproj, dval, dres),
        smem=1,
    )
    gq, gp, conv, scale = call(
        functools.partial(grad_exchange, n),
        "grad_exchange",
        [((64, 3 * D), F32), ((64, D), F32), ((18, D), F32), ((2, D), F32)],
        [
            VMEM((4, 64, 2048), BF16),
            VMEM((3, 64, 2048), BF16),
            VMEM((3, 64, 2048), BF16),
            VMEM((64, 2048), F32),
            VMEM((n, 32, 128), BF16),
            VMEM((n, 32, 128), BF16),
            VMEM((32, 128), BF16),
            VMEM((n, 32, 128), BF16),
            VMEM((8, 8, 128), F32),
            VMEM((8, 128), F32),
            VMEM((n, 8, 128), F32),
        ]
        + dma(4, 4, 3, 3, n, n, n, n, 8, 8, n, n),
        (grads, small),
        collective=2,
    )
    return out.reshape(1, 2, WIDTH, D), gq, gp, conv.reshape(2, 3, 3, D), scale


def solution(mesh):
    tokens = P("rep", "sp", None, None)
    in_specs = (tokens, tokens, P(), P(), P(), P(), P(), P(), P())
    out_specs = (tokens, P("rep", None), P("rep", None), P(), P())
    return jax.shard_map(
        functools.partial(shards, mesh.shape["sp"]),
        mesh=mesh,
        in_specs=in_specs,
        out_specs=out_specs,
        check_vma=False,
    )
```

```python
import functools

import jax
import jax.numpy as jnp
from jax import lax
from jax.experimental import pallas as pl
from jax.experimental.pallas import tpu as pltpu
from jax.sharding import PartitionSpec as P

D = 512
HEADS = 8
HEAD_DIM = 64
WIDTH = 256
EPS = 1e-06
F32 = jnp.float32
BF16 = jnp.bfloat16
TOK = 512
PAIRS = 4
VMEM = pltpu.VMEM
MESH_ID = pl.DeviceIdType.MESH
LIMIT = 60 * 1024 * 1024


def dot(a, b, ca, cb):
    return lax.dot_general(a, b, (((ca,), (cb,)), ((), ())), preferred_element_type=F32)


def ds(start, size, multiple=None):
    return pl.ds(pl.multiple_of(start, multiple or size), size)


def norm_parts(u):
    centre = jnp.mean(u, -1, keepdims=True)
    centred = u - centre
    inverse = lax.rsqrt(jnp.mean(centred * centred, -1, keepdims=True) + EPS)
    return centred * inverse, inverse


def norm_back(upstream, gain, normed, inverse):
    scaled = upstream * gain
    return inverse * (
        scaled
        - jnp.mean(scaled, -1, keepdims=True)
        - normed * jnp.mean(scaled * normed, -1, keepdims=True)
    )


def lane_low():
    return lax.broadcasted_iota(jnp.int32, (HEAD_DIM, 128), 1) < HEAD_DIM


def eye_pair():
    lane = lax.broadcasted_iota(jnp.int32, (HEAD_DIM, 128), 1)
    row = lax.broadcasted_iota(jnp.int32, (HEAD_DIM, 128), 0)
    return (lane == row) | (lane == row + HEAD_DIM)


def half_sum(v, low):
    left = jnp.sum(jnp.where(low, v, 0.0), -1, keepdims=True)
    right = jnp.sum(jnp.where(low, 0.0, v), -1, keepdims=True)
    return jnp.where(low, left, right)


def half_max(v, low):
    left = jnp.max(jnp.where(low, v, -jnp.inf), -1, keepdims=True)
    right = jnp.max(jnp.where(low, -jnp.inf, v), -1, keepdims=True)
    return jnp.where(low, left, right)


def pack_pair(full, low):
    return jnp.where(low, full[:HEAD_DIM], full[HEAD_DIM:])


def block_diag(packed, low):
    return jnp.concatenate(
        [jnp.where(low, packed, 0.0), jnp.where(low, 0.0, packed)], axis=0
    ).astype(BF16)


def pair_attention(p, gram_ref, sq_ref, sharp_ref, low, eye):
    gram = gram_ref[8 * p : 8 * p + 8].reshape(HEAD_DIM, 128)
    query_sq = half_sum(jnp.where(eye, sq_ref[p : p + 1, :], 0.0), low)
    query_norm = jnp.sqrt(query_sq + EPS)
    key_norm = jnp.sqrt(sq_ref[PAIRS + p : PAIRS + p + 1, :] + EPS)
    divisor = query_norm * key_norm
    sharp = jnp.where(low, sharp_ref[2 * p], sharp_ref[2 * p + 1])
    scores = sharp * gram / divisor
    exponent = jnp.exp(scores - half_max(scores, low))
    prob = exponent / half_sum(exponent, low)
    return prob, scores, divisor, sharp, query_norm, key_norm


def remote(src, dst, sems, at, **axes):
    return pltpu.make_async_remote_copy(
        src_ref=src,
        dst_ref=dst,
        send_sem=sems.at[0, at],
        recv_sem=sems.at[1, at],
        device_id=axes,
        device_id_type=MESH_ID,
    )


def loop(count, step, first=0):
    def go(i, _):
        step(i)
        return 0

    lax.fori_loop(first, count, go, 0)


def fold(v):
    return v.reshape(-1, 8, v.shape[-1]).sum(0)


def chunk(j):
    return slice(16 * (j // 8), 16 * (j // 8) + 16), slice(128 * (j % 8), 128 * (j % 8) + 128)


def layer(
    n,
    sharp_ref,
    x_ref,
    up_ref,
    gain1_ref,
    w_ref,
    wo_ref,
    factor_ref,
    gain2_ref,
    kern4_ref,
    out_ref,
    grads_ref,
    small_ref,
    act1_s,
    mixed_s,
    gmsg,
    ggot,
    gmine,
    gram_s,
    sq_s,
    kern_ref,
    up_halo,
    act_halo,
    dh_halo,
    act_edge,
    dh_edge,
    act_s,
    up_s,
    dh_s,
    hid_s,
    dhid_s,
    bd_s,
    att_s,
    proj_s,
    normed_s,
    inv_s,
    dact_s,
    acc_s,
    dproj_s,
    dres_s,
    datt_s,
    dmix_s,
    pmsg,
    pgot,
    pmine,
    pg_s,
    gl,
    rb1,
    sb2,
    rb2,
    acc2,
    sb3,
    rb3,
    fin,
    srb,
    ssend,
    sfin,
    s_g1,
    s_g2,
    s_p1,
    s_p2,
    s_up,
    s_act,
    s_dh,
    s_pair,
    s_col,
    s_third,
    s_fourth,
    s_small,
    s_fifth,
):
    me, rep = lax.axis_index("sp"), lax.axis_index("rep")
    reps = 8
    y, core = rep // 2, lax.rem(rep, 2)
    barrier = pltpu.get_barrier_semaphore()

    def greet(k):
        pl.semaphore_signal(
            barrier, inc=1, device_id={"sp": lax.rem(me + k, n)}, device_id_type=MESH_ID
        )

    loop(n, greet, 1)
    for k in range(1, reps):
        pl.semaphore_signal(
            barrier, inc=1, device_id={"rep": lax.rem(rep + k, reps)}, device_id_type=MESH_ID
        )
    low, eye = lane_low(), eye_pair()
    gain1, gain2 = gain1_ref[...], gain2_ref[...]
    factor0, factor1 = factor_ref[0:1, :], factor_ref[1:2, :]

    def to_above(src, halo, sems):
        return remote(src, halo.at[1], sems, 0, sp=me - 1)

    def to_below(src, halo, sems):
        return remote(src, halo.at[0], sems, 1, sp=me + 1)

    def send_above(src, halo, sems):
        @pl.when(me > 0)
        def _():
            to_above(src, halo, sems).start()

    def send_below(src, halo, sems):
        @pl.when(me < n - 1)
        def _():
            to_below(src, halo, sems).start()

    def halos_in(src, halo, sems):
        @pl.when(me > 0)
        def _():
            to_below(src, halo, sems).wait_recv()

        @pl.when(me == 0)
        def _():
            halo[0] = jnp.zeros((WIDTH, D), BF16)

        @pl.when(me < n - 1)
        def _():
            to_above(src, halo, sems).wait_recv()

        @pl.when(me == n - 1)
        def _():
            halo[1] = jnp.zeros((WIDTH, D), BF16)

    def halos_sent(src, halo, sems):
        @pl.when(me > 0)
        def _():
            to_above(src, halo, sems).wait_send()

        @pl.when(me < n - 1)
        def _():
            to_below(src, halo, sems).wait_send()

    def spread(halo, target):
        def rows(i):
            side, c = i // 4, lax.rem(i, 4)
            target[3 * side, ds(8 + c * 64, 64, 8), :] = halo[side, ds(c * 64, 64), :].astype(F32)

        loop(8, rows)

    def part_to(msg, got, sems):
        def copy(k):
            j = lax.rem(me + k, n)
            return remote(msg.at[j], got.at[k], sems, k, sp=j)

        return copy

    def part_from(mine, total, sems):
        return lambda k: remote(mine, total.at[me], sems, k, sp=lax.rem(me + k, n))

    def start_all(copy):
        loop(n, lambda k: copy(k).start(), 1)

    def add_all(copy, got, own):
        def add(k, total):
            copy(k).wait_recv()
            return total + got[k].astype(F32)

        return lax.fori_loop(1, n, add, own)

    def received(copy):
        loop(n, lambda k: copy(k).wait_recv(), 1)

    def sent(copy):
        loop(n, lambda k: copy(k).wait_send(), 1)

    def norm_one(i):
        at = ds(i * 32, 32)
        normed, _ = norm_parts(x_ref[at, :].astype(F32))
        act1_s[at, :] = (normed * gain1).astype(BF16)

    loop(TOK // 32, norm_one)

    def mix(i):
        at = ds(i * 256, 256)
        mixed_s[at, :] = dot(act1_s[at, :], w_ref[...], 1, 0).astype(BF16)

    loop(2, mix)
    lines = []
    for p in range(2 * PAIRS):
        sq = jnp.zeros((8, 128), F32)
        for i in range(0, TOK, 64):
            part = mixed_s[i : i + 64, 128 * p : 128 * p + 128].astype(F32)
            sq = sq + fold(part * part)
        lines.append(sq.sum(0, keepdims=True))
    sq = jnp.concatenate(lines, axis=0)
    for p in range(PAIRS):
        query = mixed_s[:, 128 * p : 128 * p + 128]
        key = mixed_s[:, D + 128 * p : D + 128 * p + 128]
        packed = pack_pair(dot(query, key, 0, 0), low)
        for b in range(8):
            gmsg[8 * p + b, 0:8, :] = packed[8 * b : 8 * b + 8]
    for j in range(n):
        gmsg[j, 8:16, :] = sq
    pl.semaphore_wait(barrier, n - 1 + reps - 1)
    gram_out, gram_back = part_to(gmsg, ggot, s_g1), part_from(gmine, gram_s, s_g2)
    start_all(gram_out)
    up_row = [up_ref.at[pl.ds(0, WIDTH)], up_ref.at[pl.ds(WIDTH, WIDTH)]]
    send_above(up_row[0], up_halo, s_up)
    send_below(up_row[1], up_halo, s_up)

    for at in range(18):
        kern_ref[at : at + 1, :] = kern4_ref[at // 9, (at // 3) % 3, at % 3 : at % 3 + 1, :]
    for ref, count in ((act_s, 4), (up_s, 4), (dh_s, 4), (hid_s, 2)):
        for r in range(count):
            ref[r, 0:8, :] = jnp.zeros((8, D), F32)
            ref[r, 264:272, :] = jnp.zeros((8, D), F32)
    acc_s[...] = jnp.zeros_like(acc_s)

    def upstream_rows(i):
        row, c = i // 4, lax.rem(i, 4)
        up_s[row + 1, ds(8 + c * 64, 64, 8), :] = up_ref[ds(i * 64, 64), :].astype(F32)

    loop(8, upstream_rows)
    total = add_all(gram_out, ggot, gmsg[me])
    gmine[...] = total[:8]
    start_all(gram_back)
    gram_s[me] = total[:8]
    sq_s[...] = total[8:]
    received(gram_back)

    for p in range(PAIRS):
        prob = pair_attention(p, gram_s, sq_s, sharp_ref, low, eye)[0]
        bd_s[p] = block_diag(prob, low)
    for row in range(2):
        at_row = slice(row * WIDTH, row * WIDTH + WIDTH)
        for p in range(PAIRS):
            cols = slice(128 * p, 128 * p + 128)
            value = mixed_s[at_row, 2 * D + 128 * p : 2 * D + 128 * p + 128]
            att_s[at_row, cols] = dot(value, bd_s[p], 1, 1).astype(BF16)
        proj_s[at_row, :] = dot(att_s[at_row, :], wo_ref[...], 1, 0)

        def norm_two(c, row=row):
            at = ds(row * WIDTH + c * 32, 32)
            u = x_ref[at, :].astype(F32) + factor0 * proj_s[at, :]
            normed, inverse = norm_parts(u.astype(BF16).astype(F32))
            act = (normed * gain2).astype(BF16)
            act_edge[row, ds(c * 32, 32), :] = act
            act_s[row + 1, ds(8 + c * 32, 32, 8), :] = act.astype(F32)
            normed_s[at, :] = normed
            inv_s[at, :] = jnp.broadcast_to(inverse, (32, 128))

        loop(WIDTH // 32, norm_two)
        if row == 0:
            send_above(act_edge.at[0], act_halo, s_act)
        else:
            send_below(act_edge.at[1], act_halo, s_act)

    def taps(which, lanes, i, j):
        at = 9 * which + 3 * i + j
        return kern_ref[at : at + 1, lanes]

    def place(idx):
        return ds((idx // 4) * 128, 128), lax.rem(idx, 4)

    def forth(sums):
        return pltpu.roll(sums[0], 1, 0)[8:72] + sums[1][8:72] + pltpu.roll(sums[2], 79, 0)[8:72]

    def back(sums):
        return pltpu.roll(sums[0], 79, 0)[8:72] + sums[1][8:72] + pltpu.roll(sums[2], 1, 0)[8:72]

    halos_in(up_row[0], up_halo, s_up)
    spread(up_halo, up_s)

    def hidden_grads(idx):
        r = idx // 16
        lanes, c = place(lax.rem(idx, 16))
        win = ds(c * 64, 80, 8)
        near = [up_s[r + 2 - i, win, lanes] for i in range(3)]
        scale = factor_ref[1:2, lanes]
        sums = [sum((taps(1, lanes, i, j) * scale) * near[i] for i in range(3)) for j in range(3)]
        dhid_s[ds(r * WIDTH + c * 64, 64), lanes] = back(sums)

    loop(32, hidden_grads)
    halos_in(act_edge.at[0], act_halo, s_act)
    spread(act_halo, act_s)
    for r in range(2):

        def hidden_row(idx, r=r):
            lanes, c = place(idx)
            win, mid = ds(c * 64, 80, 8), ds(8 + c * 64, 64, 8)
            near = [act_s[r + i, win, lanes] for i in range(3)]
            h = forth([sum(taps(0, lanes, i, j) * near[i] for i in range(3)) for j in range(3)])
            cumul = 0.5 * (1.0 + lax.erf(h * 0.7071067811865476))
            density = jnp.exp(-0.5 * h * h) * 0.3989422804014327
            hid_s[r, mid, lanes] = (h * cumul).astype(BF16).astype(F32)
            d_h = dhid_s[ds(r * WIDTH + c * 64, 64), lanes] * (cumul + h * density)
            dh_s[r + 1, mid, lanes] = d_h
            dh_edge[r, ds(c * 64, 64), lanes] = d_h.astype(BF16)

        loop(16, hidden_row)
        if r == 0:
            send_above(dh_edge.at[0], dh_halo, s_dh)
        else:
            send_below(dh_edge.at[1], dh_halo, s_dh)

    def kernel_grads(idx):
        r = idx // 16
        lanes, c = place(lax.rem(idx, 16))
        win, mid = ds(c * 64, 80, 8), ds(8 + c * 64, 64, 8)
        own = dh_s[r + 1, win, lanes]
        moved = [pltpu.roll(own, 79, 0)[8:72], own[8:72], pltpu.roll(own, 1, 0)[8:72]]
        for i in range(3):
            act = act_s[r + i, mid, lanes]
            for j in range(3):
                acc_s[3 * i + j, :, lanes] += fold(moved[j] * act)
        own = hid_s[r, win, lanes]
        moved = [pltpu.roll(own, 1, 0)[8:72], own[8:72], pltpu.roll(own, 79, 0)[8:72]]
        for i in range(3):
            up = up_s[r + 2 - i, mid, lanes]
            for j in range(3):
                acc_s[9 + 3 * i + j, :, lanes] += fold(moved[j] * up)

    loop(32, kernel_grads)
    halos_in(dh_edge.at[0], dh_halo, s_dh)
    spread(dh_halo, dh_s)

    def act_grads(idx):
        r = idx // 16
        lanes, c = place(lax.rem(idx, 16))
        win = ds(c * 64, 80, 8)
        near = [dh_s[r + 2 - i, win, lanes] for i in range(3)]
        sums = [sum(taps(0, lanes, i, j) * near[i] for i in range(3)) for j in range(3)]
        dact_s[ds(r * WIDTH + c * 64, 64), lanes] = back(sums)

    loop(32, act_grads)

    def residual_rows(i, scale):
        row, c = i // 8, lax.rem(i, 8)
        at = ds(i * 32, 32)
        lnb = norm_back(dact_s[at, :], gain2, normed_s[at, :], inv_s[at, 0:1])
        d_res = up_s[row + 1, ds(8 + c * 32, 32, 8), :] + lnb
        dres_s[at, :] = d_res
        dproj_s[at, :] = (factor0 * d_res).astype(BF16)
        return scale + fold(proj_s[at, :] * d_res)

    scale_one = lax.fori_loop(0, TOK // 32, residual_rows, jnp.zeros((8, D), F32))

    def attended_rows(i):
        at = ds(i * 256, 256)
        datt_s[at, :] = dot(dproj_s[at, :], wo_ref[...], 1, 1).astype(BF16)

    loop(2, attended_rows)
    for p in range(PAIRS):
        cols = slice(128 * p, 128 * p + 128)
        value = mixed_s[:, 2 * D + 128 * p : 2 * D + 128 * p + 128]
        packed = pack_pair(dot(datt_s[:, cols], value, 0, 0), low)
        for b in range(8):
            pmsg[8 * p + b, 0:8, :] = packed[8 * b : 8 * b + 8]
    lines = [acc_s[m].sum(0, keepdims=True) for m in range(18)]
    scale_two = sum(lines[9 + m] * kern_ref[9 + m : 10 + m, :] for m in range(9))
    lines = lines[:9] + [line * factor1 for line in lines[9:]]
    lines += [scale_one.sum(0, keepdims=True), scale_two]
    for j in range(n):
        pmsg[j, 8:16, :] = jnp.zeros((8, 128), F32)
    for at in range(80):
        v, b = at // 4, at % 4
        pmsg[at // 3, 8 + at % 3 : 9 + at % 3, :] = lines[v][:, 128 * b : 128 * b + 128]
    prob_out, prob_back = part_to(pmsg, pgot, s_p1), part_from(pmine, pg_s, s_p2)
    start_all(prob_out)

    def grads(half, block, left, right):
        for side in range(2):
            g = dot(left[:, 256 * side : 256 * side + 256], right, 0, 0).astype(BF16)
            for r in range(4):
                at = 4 * side + r
                gl[half, at % 2, at // 2, :, 512 * block : 512 * block + 512] = g[
                    64 * r : 64 * r + 64
                ]

    def pair_copy(half, k):
        there = lax.rem(y + 1 + k, 4)
        return remote(
            gl.at[half, 1 - core, there],
            rb1.at[half, k],
            s_pair,
            4 * half + k,
            rep=2 * y + 1 - core,
        )

    def column_copy(half, k):
        there = lax.rem(y + 1 + k, 4)
        return remote(
            sb2.at[half, k], rb2.at[half, k], s_col, 3 * half + k, rep=2 * there + core
        )

    def pair_start(half):
        for k in range(4):
            pair_copy(half, k).start()

    def pair_finish(half):
        for k in range(3):
            there = lax.rem(y + 1 + k, 4)
            pair_copy(half, k).wait_recv()

            def add(i, k=k, there=there):
                at = ds(i * 16, 16)
                sb2[half, k, at, :] = (
                    gl[half, core, there, at, :].astype(F32) + rb1[half, k, at, :].astype(F32)
                ).astype(BF16)

            loop(4, add)
            column_copy(half, k).start()
        pair_copy(half, 3).wait_recv()

        def own(i):
            at = ds(i * 16, 16)
            acc2[half, at, :] = gl[half, core, y, at, :].astype(F32) + rb1[half, 3, at, :].astype(
                F32
            )

        loop(4, own)

    def third(half):
        def copy(k):
            j = lax.rem(me + k, n)
            return remote(sb3.at[half, j], rb3.at[half, k], s_third, n * half + k, sp=j)

        return copy

    def fourth(half):
        return lambda k: remote(
            fin.at[half], grads_ref.at[half, me], s_fourth, n * half + k, sp=lax.rem(me + k, n)
        )

    def column_finish(half):
        for k in range(3):
            column_copy(half, k).wait_recv()
        for j in range(n):
            rows, cols = chunk(j)
            total = acc2[half, rows, cols]
            for k in range(3):
                total = total + rb2[half, k, rows, cols].astype(F32)
            sb3[half, j] = total.astype(BF16)
        start_all(third(half))

    def third_finish(half):
        total = add_all(third(half), rb3.at[half], sb3[half, me].astype(F32)).astype(BF16)
        fin[half] = total
        grads_ref[half, me] = total
        start_all(fourth(half))

    for p in range(PAIRS):
        cols = slice(128 * p, 128 * p + 128)
        for i in range(0, TOK, 256):
            dmix_s[i : i + 256, 2 * D + 128 * p : 2 * D + 128 * p + 128] = dot(
                datt_s[i : i + 256, cols], bd_s[p], 1, 0
            ).astype(BF16)
    grads(1, 0, act1_s, dmix_s[:, 2 * D :])
    grads(1, 1, att_s, dproj_s[...])
    pair_start(1)
    total = add_all(prob_out, pgot, pmsg[me])
    pmine[...] = total[:8]
    start_all(prob_back)
    pg_s[me] = total[:8]
    ssend[...] = total[8:]

    def small_copy(k):
        return remote(ssend, srb.at[rep], s_small, k, rep=lax.rem(rep + k, reps))

    for k in range(1, reps):
        small_copy(k).start()
    srb[rep] = total[8:]
    pair_finish(1)
    received(prob_back)

    for p in range(PAIRS):
        prob, scores, divisor, sharp, query_norm, key_norm = pair_attention(
            p, gram_s, sq_s, sharp_ref, low, eye
        )
        pg = pg_s[8 * p : 8 * p + 8].reshape(HEAD_DIM, 128)
        logit = prob * (pg - half_sum(prob * pg, low))
        bd = block_diag(logit * sharp / divisor, low)
        weighted = logit * scores
        d_qsq = -half_sum(weighted, low) / (2.0 * query_norm * query_norm)
        d_qsq = jnp.sum(jnp.where(eye, d_qsq, 0.0), 0, keepdims=True)
        d_ksq = -jnp.sum(weighted, 0, keepdims=True) / (2.0 * key_norm * key_norm)
        qc = slice(128 * p, 128 * p + 128)
        kc = slice(D + 128 * p, D + 128 * p + 128)
        for i in range(0, TOK, 256):
            at = slice(i, i + 256)
            query, key = mixed_s[at, qc], mixed_s[at, kc]
            dmix_s[at, qc] = (dot(key, bd, 1, 1) + 2.0 * d_qsq * query.astype(F32)).astype(BF16)
            dmix_s[at, kc] = (dot(query, bd, 1, 0) + 2.0 * d_ksq * key.astype(F32)).astype(BF16)
    grads(0, 0, act1_s, dmix_s[:, :D])
    grads(0, 1, act1_s, dmix_s[:, D : 2 * D])
    pair_start(0)
    column_finish(1)
    pair_finish(0)

    def inputs(i):
        at = ds(i * 256, 256)
        dact_s[at, :] = dot(dmix_s[at, :], w_ref[...], 1, 1)

    loop(2, inputs)

    def input_rows(i):
        at = ds(i * 32, 32)
        normed, inverse = norm_parts(x_ref[at, :].astype(F32))
        lnb = norm_back(dact_s[at, :], gain1, normed, inverse)
        out_ref[at, :] = (dres_s[at, :] + lnb).astype(BF16)

    loop(TOK // 32, input_rows)
    column_finish(0)
    third_finish(1)
    for k in range(1, reps):
        small_copy(k).wait_recv()
    total = srb[0]
    for k in range(1, reps):
        total = total + srb[k]
    sfin[...] = total
    small_ref[me] = total
    fifth = part_from(sfin, small_ref, s_fifth)
    start_all(fifth)
    third_finish(0)

    for copy in (gram_out, gram_back, prob_out, prob_back, third(0), third(1)):
        sent(copy)
    for src, halo, sems in (
        (up_row[0], up_halo, s_up),
        (act_edge.at[0], act_halo, s_act),
        (dh_edge.at[0], dh_halo, s_dh),
    ):
        halos_sent(src, halo, sems)
    for k in range(1, reps):
        small_copy(k).wait_send()
    for half in range(2):
        for k in range(4):
            pair_copy(half, k).wait_send()
        for k in range(3):
            column_copy(half, k).wait_send()
    for copy in (fourth(1), fifth, fourth(0)):
        received(copy)
        sent(copy)


def finish(out_in, grads_ref, small_ref, out_ref, gq_ref, gp_ref, conv_ref, scale_ref):
    out_ref[...] = out_in[...]
    for j in range(32):
        rows, cols = chunk(j)
        gq_ref[rows, cols] = grads_ref[0, j].astype(F32)
        if cols.start < D:
            gq_ref[rows, 2 * D + cols.start : 2 * D + cols.stop] = grads_ref[1, j].astype(F32)
        else:
            gp_ref[rows, cols.start - D : cols.stop - D] = grads_ref[1, j].astype(F32)
    for at in range(80):
        v, b = at // 4, at % 4
        line = small_ref[at // 3, at % 3 : at % 3 + 1, :]
        lanes = slice(128 * b, 128 * b + 128)
        if v < 18:
            conv_ref[v // 9, (v // 3) % 3, v % 3 : v % 3 + 1, lanes] = line
        else:
            scale_ref[v - 18 : v - 17, lanes] = line


def call(body, name, outs, scratch, args, smem=0, collective=None):
    params = dict(vmem_limit_bytes=LIMIT)
    if collective is not None:
        params.update(collective_id=collective, has_side_effects=True)
    specs = [pl.BlockSpec(memory_space=pltpu.SMEM)] * smem
    specs += [pl.BlockSpec(memory_space=VMEM)] * (len(args) - smem)
    return pl.pallas_call(
        body,
        name=name,
        out_shape=[jax.ShapeDtypeStruct(s, t) for s, t in outs],
        in_specs=specs,
        out_specs=[pl.BlockSpec(memory_space=VMEM)] * len(outs),
        scratch_shapes=scratch,
        compiler_params=pltpu.CompilerParams(**params),
    )(*args)


def shards(n, x, up, gain1, w, sharp, wo, factors, gain2, kernels):
    x = x.reshape(TOK, D)
    up = up.reshape(TOK, D)
    gain1, gain2 = gain1.reshape(1, D), gain2.reshape(1, D)
    scratch = [
        VMEM((TOK, D), BF16),
        VMEM((TOK, 3 * D), BF16),
        VMEM((n, 16, 128), F32),
        VMEM((n, 16, 128), F32),
        VMEM((8, 128), F32),
        VMEM((n, 8, 128), F32),
        VMEM((8, 128), F32),
        VMEM((18, D), F32),
        VMEM((2, WIDTH, D), BF16),
        VMEM((2, WIDTH, D), BF16),
        VMEM((2, WIDTH, D), BF16),
        VMEM((2, WIDTH, D), BF16),
        VMEM((2, WIDTH, D), BF16),
        VMEM((4, 272, D), F32),
        VMEM((4, 272, D), F32),
        VMEM((4, 272, D), F32),
        VMEM((2, 272, D), F32),
        VMEM((TOK, D), F32),
        VMEM((PAIRS, 128, 128), BF16),
        VMEM((TOK, D), BF16),
        VMEM((TOK, D), F32),
        VMEM((TOK, D), F32),
        VMEM((TOK, 128), F32),
        VMEM((TOK, D), F32),
        VMEM((18, 8, D), F32),
        VMEM((TOK, D), BF16),
        VMEM((TOK, D), F32),
        VMEM((TOK, D), BF16),
        VMEM((TOK, 3 * D), BF16),
        VMEM((n, 16, 128), F32),
        VMEM((n, 16, 128), F32),
        VMEM((8, 128), F32),
        VMEM((n, 8, 128), F32),
        VMEM((2, 2, 4, 64, 1024), BF16),
        VMEM((2, 4, 64, 1024), BF16),
        VMEM((2, 3, 64, 1024), BF16),
        VMEM((2, 3, 64, 1024), BF16),
        VMEM((2, 64, 1024), F32),
        VMEM((2, n, 16, 128), BF16),
        VMEM((2, n, 16, 128), BF16),
        VMEM((2, 16, 128), BF16),
        VMEM((8, 8, 128), F32),
        VMEM((8, 128), F32),
        VMEM((8, 128), F32),
    ]
    for count in (n, n, n, n, 2, 2, 2, 8, 6, 2 * n, 2 * n, 8, n):
        scratch.append(pltpu.SemaphoreType.DMA((2, count)))
    out, grads, small = call(
        functools.partial(layer, n),
        "layer",
        [((TOK, D), BF16), ((2, n, 16, 128), BF16), ((n, 8, 128), F32)],
        scratch,
        (sharp, x, up, gain1, w, wo, factors, gain2, kernels),
        smem=1,
        collective=0,
    )
    out, gq, gp, conv, scale = call(
        finish,
        "finish",
        [
            ((TOK, D), BF16),
            ((64, 3 * D), F32),
            ((64, D), F32),
            ((2, 3, 3, D), F32),
            ((2, D), F32),
        ],
        [],
        (out, grads, small),
    )
    return out.reshape(1, 2, WIDTH, D), gq, gp, conv, scale


def solution(mesh):
    tokens = P("rep", "sp", None, None)
    in_specs = (tokens, tokens, P(), P(), P(), P(), P(), P(), P())
    out_specs = (tokens, P("rep", None), P("rep", None), P(), P())
    return jax.shard_map(
        functools.partial(shards, mesh.shape["sp"]),
        mesh=mesh,
        in_specs=in_specs,
        out_specs=out_specs,
        check_vma=False,
    )
```

```python
import functools

import jax
import jax.numpy as jnp
from jax import lax
from jax.experimental import pallas as pl
from jax.experimental.pallas import tpu as pltpu
from jax.sharding import PartitionSpec as P

D = 512
HEADS = 8
HEAD_DIM = 64
WIDTH = 256
EPS = 1e-06
F32 = jnp.float32
BF16 = jnp.bfloat16
TOK = 512
PAIRS = 4
VMEM = pltpu.VMEM
MESH_ID = pl.DeviceIdType.MESH
LIMIT = 60 * 1024 * 1024


def dot(a, b, ca, cb):
    return lax.dot_general(a, b, (((ca,), (cb,)), ((), ())), preferred_element_type=F32)


def ds(start, size, multiple=None):
    return pl.ds(pl.multiple_of(start, multiple or size), size)


def norm_parts(u):
    centre = jnp.mean(u, -1, keepdims=True)
    centred = u - centre
    inverse = lax.rsqrt(jnp.mean(centred * centred, -1, keepdims=True) + EPS)
    return centred * inverse, inverse


def norm_back(upstream, gain, normed, inverse):
    scaled = upstream * gain
    return inverse * (
        scaled
        - jnp.mean(scaled, -1, keepdims=True)
        - normed * jnp.mean(scaled * normed, -1, keepdims=True)
    )


def lane_low():
    return lax.broadcasted_iota(jnp.int32, (HEAD_DIM, 128), 1) < HEAD_DIM


def eye_pair():
    lane = lax.broadcasted_iota(jnp.int32, (HEAD_DIM, 128), 1)
    row = lax.broadcasted_iota(jnp.int32, (HEAD_DIM, 128), 0)
    return (lane == row) | (lane == row + HEAD_DIM)


def half_sum(v, low):
    left = jnp.sum(jnp.where(low, v, 0.0), -1, keepdims=True)
    right = jnp.sum(jnp.where(low, 0.0, v), -1, keepdims=True)
    return jnp.where(low, left, right)


def half_max(v, low):
    left = jnp.max(jnp.where(low, v, -jnp.inf), -1, keepdims=True)
    right = jnp.max(jnp.where(low, -jnp.inf, v), -1, keepdims=True)
    return jnp.where(low, left, right)


def pack_pair(full, low):
    return jnp.where(low, full[:HEAD_DIM], full[HEAD_DIM:])


def block_diag(packed, low):
    return jnp.concatenate(
        [jnp.where(low, packed, 0.0), jnp.where(low, 0.0, packed)], axis=0
    ).astype(BF16)


def pair_attention(p, gram_ref, sq_ref, sharp_ref, low, eye):
    gram = gram_ref[8 * p : 8 * p + 8].reshape(HEAD_DIM, 128)
    query_sq = half_sum(jnp.where(eye, sq_ref[p : p + 1, :], 0.0), low)
    query_norm = jnp.sqrt(query_sq + EPS)
    key_norm = jnp.sqrt(sq_ref[PAIRS + p : PAIRS + p + 1, :] + EPS)
    divisor = query_norm * key_norm
    sharp = jnp.where(low, sharp_ref[2 * p], sharp_ref[2 * p + 1])
    scores = sharp * gram / divisor
    exponent = jnp.exp(scores - half_max(scores, low))
    prob = exponent / half_sum(exponent, low)
    return prob, scores, divisor, sharp, query_norm, key_norm


def remote(src, dst, sems, at, **axes):
    return pltpu.make_async_remote_copy(
        src_ref=src,
        dst_ref=dst,
        send_sem=sems.at[0, at],
        recv_sem=sems.at[1, at],
        device_id=axes,
        device_id_type=MESH_ID,
    )


def loop(count, step, first=0, each=1):
    def go(i, _):
        for u in range(each):
            step(i * each + u)
        return 0

    lax.fori_loop(first, count // each, go, 0)


def fold(v):
    return v.reshape(-1, 8, v.shape[-1]).sum(0)


def chunk(j):
    return slice(16 * (j // 8), 16 * (j // 8) + 16), slice(128 * (j % 8), 128 * (j % 8) + 128)


def layer(
    n,
    sharp_ref,
    x_ref,
    up_hbm,
    gain1_ref,
    w_hbm,
    wo_hbm,
    factor_ref,
    gain2_ref,
    kern4_ref,
    out_ref,
    grads_ref,
    small_ref,
    up_ref,
    w_ref,
    wo_ref,
    act1_s,
    mixed_s,
    gmsg,
    ggot,
    gmine,
    gram_s,
    gsq,
    gsqgot,
    gsqmine,
    sq_all,
    sq_s,
    kern_ref,
    up_halo,
    act_halo,
    dh_halo,
    act_edge,
    dh_edge,
    act_s,
    up_s,
    dh_s,
    hid_s,
    dhid_s,
    bd_s,
    bd2_s,
    att_s,
    proj_s,
    normed_s,
    inv_s,
    dact_s,
    acc_s,
    dproj_s,
    dres_s,
    datt_s,
    dmix_s,
    pmsg,
    pgot,
    pmine,
    pg_s,
    smsg,
    sgot,
    pm_s,
    actp_s,
    mbuf,
    mgot,
    mtot,
    qs,
    qgot,
    gl,
    rb1,
    sb2,
    rb2,
    acc2,
    sb3,
    rb3,
    fin,
    srb,
    ssend,
    sfin,
    s_load,
    s_g1,
    s_g2,
    s_q1,
    s_q2,
    s_p1,
    s_p2,
    s_s1,
    s_up,
    s_act,
    s_dh,
    s_m,
    s_qx,
    s_pair,
    s_col,
    s_third,
    s_fourth,
    s_small,
    s_fifth,
):
    me, rep = lax.axis_index("sp"), lax.axis_index("rep")
    reps = 8
    loads = [
        pltpu.make_async_copy(src, dst, s_load.at[0, at])
        for at, (src, dst) in enumerate(((w_hbm, w_ref), (up_hbm, up_ref), (wo_hbm, wo_ref)))
    ]
    for load in loads:
        load.start()
    y, core = rep // 2, lax.rem(rep, 2)
    barrier = pltpu.get_barrier_semaphore()

    def greet(k):
        pl.semaphore_signal(
            barrier, inc=1, device_id={"sp": lax.rem(me + k, n)}, device_id_type=MESH_ID
        )

    loop(n, greet, 1)
    for k in range(1, reps):
        pl.semaphore_signal(
            barrier, inc=1, device_id={"rep": lax.rem(rep + k, reps)}, device_id_type=MESH_ID
        )
    low, eye = lane_low(), eye_pair()
    gain1, gain2 = gain1_ref[...], gain2_ref[...]
    factor0, factor1 = factor_ref[0:1, :], factor_ref[1:2, :]

    def to_above(src, halo, sems):
        return remote(src, halo.at[1], sems, 0, sp=me - 1)

    def to_below(src, halo, sems):
        return remote(src, halo.at[0], sems, 1, sp=me + 1)

    def send_above(src, halo, sems):
        @pl.when(me > 0)
        def _():
            to_above(src, halo, sems).start()

    def send_below(src, halo, sems):
        @pl.when(me < n - 1)
        def _():
            to_below(src, halo, sems).start()

    def halos_in(src, halo, sems):
        @pl.when(me > 0)
        def _():
            to_below(src, halo, sems).wait_recv()

        @pl.when(me == 0)
        def _():
            halo[0] = jnp.zeros((WIDTH, D), BF16)

        @pl.when(me < n - 1)
        def _():
            to_above(src, halo, sems).wait_recv()

        @pl.when(me == n - 1)
        def _():
            halo[1] = jnp.zeros((WIDTH, D), BF16)

    def halos_sent(src, halo, sems):
        @pl.when(me > 0)
        def _():
            to_above(src, halo, sems).wait_send()

        @pl.when(me < n - 1)
        def _():
            to_below(src, halo, sems).wait_send()

    def spread(halo, target):
        def rows(i):
            side, c = i // 4, lax.rem(i, 4)
            target[3 * side, ds(8 + c * 64, 64, 8), :] = halo[side, ds(c * 64, 64), :].astype(F32)

        loop(8, rows)

    def part_to(msg, got, sems):
        def copy(k):
            j = lax.rem(me + k, n)
            return remote(msg.at[j], got.at[k], sems, k, sp=j)

        return copy

    def part_from(mine, total, sems):
        return lambda k: remote(mine, total.at[me], sems, k, sp=lax.rem(me + k, n))

    def start_all(*copies):
        def start(k):
            for copy in copies:
                copy(k).start()

        loop(n, start, 1)

    def add_all(copy, got, own):
        def add(k, total):
            copy(k).wait_recv()
            return total + got[k].astype(F32)

        return lax.fori_loop(1, n, add, own)

    def received(copy):
        loop(n, lambda k: copy(k).wait_recv(), 1)

    def sent(copy):
        loop(n, lambda k: copy(k).wait_send(), 1)

    def norm_one(i):
        at = ds(i * 32, 32)
        normed, _ = norm_parts(x_ref[at, :].astype(F32))
        act1_s[at, :] = (normed * gain1).astype(BF16)

    loop(TOK // 32, norm_one, each=4)
    loads[0].wait()

    def mix(i):
        at = ds(i * 256, 256)
        mixed_s[at, :] = dot(act1_s[at, :], w_ref[...], 1, 0).astype(BF16)

    loop(2, mix)
    lines = []
    for p in range(2 * PAIRS):
        sq = jnp.zeros((8, 128), F32)
        for i in range(0, TOK, 64):
            part = mixed_s[i : i + 64, 128 * p : 128 * p + 128].astype(F32)
            sq = sq + fold(part * part)
        lines.append(sq.sum(0, keepdims=True))
    sq = jnp.concatenate(lines, axis=0)
    for p in range(PAIRS):
        query = mixed_s[:, 128 * p : 128 * p + 128]
        key = mixed_s[:, D + 128 * p : D + 128 * p + 128]
        packed = pack_pair(dot(query, key, 0, 0), low)
        for b in range(8):
            gmsg[8 * p + b] = packed[8 * b : 8 * b + 8]
    quarter = lax.broadcasted_iota(jnp.int32, (1, 128), 1) >> 5
    for j in range(n):
        gsq[j] = jnp.where(quarter == j % 4, sq[j // 4 : j // 4 + 1], 0.0)
    pl.semaphore_wait(barrier, n - 1 + reps - 1)
    gram_out, gram_back = part_to(gmsg, ggot, s_g1), part_from(gmine, gram_s, s_g2)
    sq_out, sq_back = part_to(gsq, gsqgot, s_q1), part_from(gsqmine, sq_all, s_q2)
    start_all(gram_out, sq_out)
    up_row = [up_ref.at[pl.ds(0, WIDTH)], up_ref.at[pl.ds(WIDTH, WIDTH)]]

    def product_copy(p):
        def copy(k):
            j = lax.rem(me + k, n)
            return remote(mbuf.at[p, j], mgot.at[p, k], s_m, n * p + k, sp=j)

        return copy

    def product(p):
        for at in range(2):
            cols = slice(512 * at + 128 * p, 512 * at + 128 * p + 128)
            part = dot(actp_s[...], mixed_s[:, cols], 0, 0).astype(BF16)
            mbuf[p, :, :, 128 * at : 128 * at + 128] = part.reshape(n, 16, 128)

    lane = lax.broadcasted_iota(jnp.int32, (64, D), 1)
    line = lax.broadcasted_iota(jnp.int32, (64, D), 0)
    spot = (line >> 1) * 16 + (line & 1)
    for r in range(8):
        pm_s[64 * r : 64 * r + 64, :] = jnp.where(lane == spot + 2 * r, 1.0, 0.0).astype(BF16)
    for i in range(0, TOK, 256):
        actp_s[i : i + 256, :] = dot(act1_s[i : i + 256, :], pm_s[...], 1, 0).astype(BF16)
    product(0)
    start_all(product_copy(0))
    for p in range(1, PAIRS):
        product(p)

    for at in range(18):
        kern_ref[at : at + 1, :] = kern4_ref[(at // 3) % 3, at % 3, at // 9 : at // 9 + 1, :]
    for ref, count in ((act_s, 4), (up_s, 4), (dh_s, 4), (hid_s, 2)):
        for r in range(count):
            ref[r, 0:8, :] = jnp.zeros((8, D), F32)
            ref[r, 264:272, :] = jnp.zeros((8, D), F32)
    acc_s[...] = jnp.zeros_like(acc_s)

    def upstream_rows(i):
        row, c = i // 4, lax.rem(i, 4)
        up_s[row + 1, ds(8 + c * 64, 64, 8), :] = up_ref[ds(i * 64, 64), :].astype(F32)

    loads[1].wait()
    loop(8, upstream_rows)
    total = add_all(gram_out, ggot, gmsg[me])
    gmine[...] = total
    gram_s[me] = total
    total = add_all(sq_out, gsqgot, gsq[me])
    gsqmine[...] = total
    sq_all[me] = total
    start_all(gram_back, sq_back)
    send_above(up_row[0], up_halo, s_up)
    send_below(up_row[1], up_halo, s_up)
    start_all(product_copy(1))
    start_all(product_copy(3))
    loads[2].wait()
    received(gram_back)
    received(sq_back)
    for p in range(2 * PAIRS):
        sq_s[p : p + 1, :] = sq_all[4 * p] + sq_all[4 * p + 1] + sq_all[4 * p + 2] + sq_all[4 * p + 3]

    for p in range(PAIRS):
        prob = pair_attention(p, gram_s, sq_s, sharp_ref, low, eye)[0]
        bd_s[p] = block_diag(prob, low)
    for row in range(2):
        at_row = slice(row * WIDTH, row * WIDTH + WIDTH)
        for p in range(PAIRS):
            cols = slice(128 * p, 128 * p + 128)
            value = mixed_s[at_row, 2 * D + 128 * p : 2 * D + 128 * p + 128]
            att_s[at_row, cols] = dot(value, bd_s[p], 1, 1).astype(BF16)
        proj_s[at_row, :] = dot(att_s[at_row, :], wo_ref[...], 1, 0)

        def norm_two(c, row=row):
            at = ds(row * WIDTH + c * 32, 32)
            u = x_ref[at, :].astype(F32) + factor0 * proj_s[at, :]
            normed, inverse = norm_parts(u.astype(BF16).astype(F32))
            act = (normed * gain2).astype(BF16)
            act_edge[row, ds(c * 32, 32), :] = act
            act_s[row + 1, ds(8 + c * 32, 32, 8), :] = act.astype(F32)
            normed_s[at, :] = normed
            inv_s[at, :] = jnp.broadcast_to(inverse, (32, 128))

        loop(WIDTH // 32, norm_two, each=4)
        if row == 0:
            send_above(act_edge.at[0], act_halo, s_act)
        else:
            send_below(act_edge.at[1], act_halo, s_act)

    def taps(which, lanes, i, j):
        at = 9 * which + 3 * i + j
        return kern_ref[at : at + 1, lanes]

    def place(idx):
        return ds((idx // 4) * 128, 128), lax.rem(idx, 4)

    def forth(sums):
        return pltpu.roll(sums[0], 1, 0)[8:72] + sums[1][8:72] + pltpu.roll(sums[2], 79, 0)[8:72]

    def back(sums):
        return pltpu.roll(sums[0], 79, 0)[8:72] + sums[1][8:72] + pltpu.roll(sums[2], 1, 0)[8:72]

    halos_in(up_row[0], up_halo, s_up)
    spread(up_halo, up_s)

    def hidden_grads(idx):
        r = idx // 16
        lanes, c = place(lax.rem(idx, 16))
        win = ds(c * 64, 80, 8)
        near = [up_s[r + 2 - i, win, lanes] for i in range(3)]
        scale = factor_ref[1:2, lanes]
        sums = [sum((taps(1, lanes, i, j) * scale) * near[i] for i in range(3)) for j in range(3)]
        dhid_s[ds(r * WIDTH + c * 64, 64), lanes] = back(sums)

    loop(32, hidden_grads)
    halos_in(act_edge.at[0], act_halo, s_act)
    spread(act_halo, act_s)
    for r in range(2):

        def hidden_row(idx, r=r):
            lanes, c = place(idx)
            win, mid = ds(c * 64, 80, 8), ds(8 + c * 64, 64, 8)
            near = [act_s[r + i, win, lanes] for i in range(3)]
            h = forth([sum(taps(0, lanes, i, j) * near[i] for i in range(3)) for j in range(3)])
            cumul = 0.5 * (1.0 + lax.erf(h * 0.7071067811865476))
            density = jnp.exp(-0.5 * h * h) * 0.3989422804014327
            hid_s[r, mid, lanes] = (h * cumul).astype(BF16).astype(F32)
            d_h = dhid_s[ds(r * WIDTH + c * 64, 64), lanes] * (cumul + h * density)
            dh_s[r + 1, mid, lanes] = d_h
            dh_edge[r, ds(c * 64, 64), lanes] = d_h.astype(BF16)

        loop(16, hidden_row)
        if r == 0:
            send_above(dh_edge.at[0], dh_halo, s_dh)
        else:
            send_below(dh_edge.at[1], dh_halo, s_dh)
    start_all(product_copy(2))

    def kernel_grads(idx):
        r = idx // 16
        lanes, c = place(lax.rem(idx, 16))
        win, mid = ds(c * 64, 80, 8), ds(8 + c * 64, 64, 8)
        own = dh_s[r + 1, win, lanes]
        moved = [pltpu.roll(own, 79, 0)[8:72], own[8:72], pltpu.roll(own, 1, 0)[8:72]]
        for i in range(3):
            act = act_s[r + i, mid, lanes]
            for j in range(3):
                acc_s[3 * i + j, :, lanes] += fold(moved[j] * act)
        own = hid_s[r, win, lanes]
        moved = [pltpu.roll(own, 1, 0)[8:72], own[8:72], pltpu.roll(own, 79, 0)[8:72]]
        for i in range(3):
            up = up_s[r + 2 - i, mid, lanes]
            for j in range(3):
                acc_s[9 + 3 * i + j, :, lanes] += fold(moved[j] * up)

    loop(32, kernel_grads)
    halos_in(dh_edge.at[0], dh_halo, s_dh)
    spread(dh_halo, dh_s)

    def act_grads(idx):
        r = idx // 16
        lanes, c = place(lax.rem(idx, 16))
        win = ds(c * 64, 80, 8)
        near = [dh_s[r + 2 - i, win, lanes] for i in range(3)]
        sums = [sum(taps(0, lanes, i, j) * near[i] for i in range(3)) for j in range(3)]
        dact_s[ds(r * WIDTH + c * 64, 64), lanes] = back(sums)

    loop(32, act_grads)

    def residual_rows(step, scale):
        for u in range(4):
            i = 4 * step + u
            row, c = i // 8, lax.rem(i, 8)
            at = ds(i * 32, 32)
            lnb = norm_back(dact_s[at, :], gain2, normed_s[at, :], inv_s[at, 0:1])
            d_res = up_s[row + 1, ds(8 + c * 32, 32, 8), :] + lnb
            dres_s[at, :] = d_res
            dproj_s[at, :] = (factor0 * d_res).astype(BF16)
            scale = scale + fold(proj_s[at, :] * d_res)
        return scale

    scale_one = lax.fori_loop(0, TOK // 128, residual_rows, jnp.zeros((8, D), F32))

    def attended_rows(i):
        at = ds(i * 256, 256)
        datt_s[at, :] = dot(dproj_s[at, :], wo_ref[...], 1, 1).astype(BF16)

    loop(2, attended_rows)
    for p in range(PAIRS):
        cols = slice(128 * p, 128 * p + 128)
        value = mixed_s[:, 2 * D + 128 * p : 2 * D + 128 * p + 128]
        packed = pack_pair(dot(datt_s[:, cols], value, 0, 0), low)
        for b in range(8):
            pmsg[8 * p + b] = packed[8 * b : 8 * b + 8]
    prob_out, prob_back = part_to(pmsg, pgot, s_p1), part_from(pmine, pg_s, s_p2)
    start_all(prob_out)
    lines = [acc_s[m].sum(0, keepdims=True) for m in range(18)]
    scale_two = sum(lines[9 + m] * kern_ref[9 + m : 10 + m, :] for m in range(9))
    lines = lines[:9] + [line * factor1 for line in lines[9:]]
    lines += [scale_one.sum(0, keepdims=True), scale_two]
    smsg[...] = jnp.zeros_like(smsg)
    for at in range(80):
        v, b = at // 4, at % 4
        smsg[at // 3, at % 3 : at % 3 + 1, :] = lines[v][:, 128 * b : 128 * b + 128]
    small_out = part_to(smsg, sgot, s_s1)
    start_all(small_out)

    def grads(block, left, right):
        for side in range(2):
            g = dot(left[:, 256 * side : 256 * side + 256], right, 0, 0).astype(BF16)
            for r in range(4):
                at = 4 * side + r
                gl[at % 2, at // 2, :, 512 * block : 512 * block + 512] = g[64 * r : 64 * r + 64]

    def pair_copy(k):
        there = lax.rem(y + 1 + k, 4)
        return remote(gl.at[1 - core, there], rb1.at[k], s_pair, k, rep=2 * y + 1 - core)

    def column_copy(k):
        there = lax.rem(y + 1 + k, 4)
        return remote(sb2.at[k], rb2.at[k], s_col, k, rep=2 * there + core)

    def pair_finish():
        for k in range(3):
            there = lax.rem(y + 1 + k, 4)
            pair_copy(k).wait_recv()

            def add(i, k=k, there=there):
                at = ds(i * 16, 16)
                sb2[k, at, :] = (
                    gl[core, there, at, :].astype(F32) + rb1[k, at, :].astype(F32)
                ).astype(BF16)

            loop(4, add)
            column_copy(k).start()
        pair_copy(3).wait_recv()

        def own(i):
            at = ds(i * 16, 16)
            acc2[at, :] = gl[core, y, at, :].astype(F32) + rb1[3, at, :].astype(F32)

        loop(4, own)

    def third(k):
        j = lax.rem(me + k, n)
        return remote(sb3.at[j], rb3.at[k], s_third, k, sp=j)

    def fourth(half):
        return lambda k: remote(
            fin.at[half], grads_ref.at[half, me], s_fourth, n * half + k, sp=lax.rem(me + k, n)
        )

    def column_finish():
        for k in range(3):
            column_copy(k).wait_recv()
        for j in range(n):
            rows, cols = chunk(j)
            total = acc2[rows, cols]
            for k in range(3):
                total = total + rb2[k, rows, cols].astype(F32)
            sb3[j] = total.astype(BF16)
        start_all(third)

    def to_everyone(half, total):
        fin[half] = total.astype(BF16)
        grads_ref[half, me] = total.astype(BF16)
        start_all(fourth(half))

    for p in range(PAIRS):
        cols = slice(128 * p, 128 * p + 128)
        for i in range(0, TOK, 256):
            dmix_s[i : i + 256, 2 * D + 128 * p : 2 * D + 128 * p + 128] = dot(
                datt_s[i : i + 256, cols], bd_s[p], 1, 0
            ).astype(BF16)
    grads(0, act1_s, dmix_s[:, 2 * D :])
    grads(1, att_s, dproj_s[...])
    for k in range(4):
        pair_copy(k).start()
    for p in range(PAIRS):
        total = add_all(product_copy(p), mgot.at[p], mbuf[p, me].astype(F32))
        mtot[:, 128 * p : 128 * p + 128] = total[:, :128]
        mtot[:, D + 128 * p : D + 128 * p + 128] = total[:, 128:]
    pair_finish()
    total = add_all(prob_out, pgot, pmsg[me])
    pmine[...] = total
    start_all(prob_back)
    pg_s[me] = total
    total = add_all(small_out, sgot, smsg[me])
    ssend[...] = total
    srb[rep] = total

    def small_copy(k):
        return remote(ssend, srb.at[rep], s_small, k, rep=lax.rem(rep + k, reps))

    for k in range(1, reps):
        small_copy(k).start()
    column_finish()
    received(prob_back)

    def split_dot(a, b, ca, cb):
        high = a.astype(BF16)
        rest = (a - high.astype(F32)).astype(BF16)
        return dot(high, b, ca, cb) + dot(rest, b, ca, cb)

    squares = []
    for p in range(PAIRS):
        prob, scores, divisor, sharp, query_norm, key_norm = pair_attention(
            p, gram_s, sq_s, sharp_ref, low, eye
        )
        pg = pg_s[8 * p : 8 * p + 8].reshape(HEAD_DIM, 128)
        logit = prob * (pg - half_sum(prob * pg, low))
        bd2_s[p] = block_diag(logit * sharp / divisor, low)
        weighted = logit * scores
        d_qsq = -half_sum(weighted, low) / (2.0 * query_norm * query_norm)
        d_qsq = 2.0 * jnp.sum(jnp.where(eye, d_qsq, 0.0), 0, keepdims=True)
        d_ksq = -2.0 * jnp.sum(weighted, 0, keepdims=True) / (2.0 * key_norm * key_norm)
        squares.append((d_qsq, d_ksq))
        by_query = mtot[:, 128 * p : 128 * p + 128]
        by_key = mtot[:, D + 128 * p : D + 128 * p + 128]
        g_query = split_dot(by_key, bd2_s[p], 1, 1) + d_qsq * by_query
        g_key = split_dot(by_query, bd2_s[p], 1, 0) + d_ksq * by_key
        for r in range(reps):
            qs[r, 2 * p : 2 * p + 2, :] = g_query[2 * r : 2 * r + 2]
            qs[r, 8 + 2 * p : 10 + 2 * p, :] = g_key[2 * r : 2 * r + 2]

    def query_copy(k):
        there = lax.rem(rep + k, reps)
        return remote(qs.at[there], qgot.at[rep], s_qx, k, rep=there)

    for k in range(1, reps):
        query_copy(k).start()
    qgot[rep] = qs[rep]
    for p in range(PAIRS):
        d_qsq, d_ksq = squares[p]
        qc = slice(128 * p, 128 * p + 128)
        kc = slice(D + 128 * p, D + 128 * p + 128)
        for i in range(0, TOK, 256):
            at = slice(i, i + 256)
            query, key = mixed_s[at, qc], mixed_s[at, kc]
            dmix_s[at, qc] = (dot(key, bd2_s[p], 1, 1) + d_qsq * query.astype(F32)).astype(BF16)
            dmix_s[at, kc] = (dot(query, bd2_s[p], 1, 0) + d_ksq * key.astype(F32)).astype(BF16)

    def inputs(i):
        at = ds(i * 256, 256)
        dact_s[at, :] = dot(dmix_s[at, :], w_ref[...], 1, 1)

    loop(2, inputs)
    for k in range(1, reps):
        query_copy(k).wait_recv()
    total = qgot[0]
    for k in range(1, reps):
        total = total + qgot[k]
    to_everyone(0, total)
    for k in range(1, reps):
        small_copy(k).wait_recv()
    total = srb[0]
    for k in range(1, reps):
        total = total + srb[k]
    sfin[...] = total
    small_ref[me] = total
    fifth = part_from(sfin, small_ref, s_fifth)
    start_all(fifth)
    to_everyone(1, add_all(third, rb3, sb3[me].astype(F32)))

    def input_rows(i):
        at = ds(i * 32, 32)
        normed, inverse = norm_parts(x_ref[at, :].astype(F32))
        lnb = norm_back(dact_s[at, :], gain1, normed, inverse)
        out_ref[at, :] = (dres_s[at, :] + lnb).astype(BF16)

    loop(TOK // 32, input_rows, each=4)

    for copy in (gram_out, gram_back, sq_out, sq_back, prob_out, prob_back, small_out, third):
        sent(copy)
    for p in range(PAIRS):
        sent(product_copy(p))
    for src, halo, sems in (
        (up_row[0], up_halo, s_up),
        (act_edge.at[0], act_halo, s_act),
        (dh_edge.at[0], dh_halo, s_dh),
    ):
        halos_sent(src, halo, sems)
    for k in range(1, reps):
        small_copy(k).wait_send()
        query_copy(k).wait_send()
    for k in range(4):
        pair_copy(k).wait_send()
    for k in range(3):
        column_copy(k).wait_send()
    for copy in (fourth(0), fifth, fourth(1)):
        received(copy)
        sent(copy)


def finish(out_in, grads_ref, small_ref, out_ref, gq_ref, gp_ref, conv_ref, scale_ref):
    out_ref[...] = out_in[...]
    for j in range(32):
        rows, cols = chunk(j)
        own = grads_ref[0, j].astype(F32)
        for q in range(8):
            gq_ref[2 * j : 2 * j + 2, 128 * q : 128 * q + 128] = own[2 * q : 2 * q + 2]
        if cols.start < D:
            gq_ref[rows, 2 * D + cols.start : 2 * D + cols.stop] = grads_ref[1, j].astype(F32)
        else:
            gp_ref[rows, cols.start - D : cols.stop - D] = grads_ref[1, j].astype(F32)
    for at in range(80):
        v, b = at // 4, at % 4
        line = small_ref[at // 3, at % 3 : at % 3 + 1, :]
        lanes = slice(128 * b, 128 * b + 128)
        if v < 18:
            conv_ref[(v // 3) % 3, v % 3, v // 9 : v // 9 + 1, lanes] = line
        else:
            scale_ref[v - 18 : v - 17, lanes] = line


def call(body, name, outs, scratch, args, smem=0, collective=None, away=()):
    params = dict(vmem_limit_bytes=LIMIT)
    if collective is not None:
        params.update(collective_id=collective, has_side_effects=True)
    specs = [pl.BlockSpec(memory_space=pltpu.SMEM)] * smem
    specs += [
        pl.BlockSpec(memory_space=pl.ANY if at in away else VMEM) for at in range(smem, len(args))
    ]
    return pl.pallas_call(
        body,
        name=name,
        out_shape=[jax.ShapeDtypeStruct(s, t) for s, t in outs],
        in_specs=specs,
        out_specs=[pl.BlockSpec(memory_space=VMEM)] * len(outs),
        scratch_shapes=scratch,
        compiler_params=pltpu.CompilerParams(**params),
    )(*args)


def shards(n, x, up, gain1, w, sharp, wo, factors, gain2, kernels):
    x = x.reshape(TOK, D)
    up = up.reshape(TOK, D)
    gain1, gain2 = gain1.reshape(1, D), gain2.reshape(1, D)
    kernels = kernels.transpose(1, 2, 0, 3)
    row = VMEM((n, 8, 128), F32)
    edge = VMEM((2, WIDTH, D), BF16)
    wide, tall = VMEM((TOK, D), BF16), VMEM((TOK, D), F32)
    scratch = [wide, VMEM((D, 3 * D), BF16), wide, wide, VMEM((TOK, 3 * D), BF16)]
    scratch += [row, row, VMEM((8, 128), F32), row]
    scratch += [VMEM((n, 1, 128), F32), VMEM((n, 1, 128), F32), VMEM((1, 128), F32)]
    scratch += [VMEM((n, 1, 128), F32), VMEM((8, 128), F32), VMEM((18, D), F32)]
    scratch += [edge] * 5
    scratch += [VMEM((count, 272, D), F32) for count in (4, 4, 4, 2)]
    scratch += [tall, VMEM((PAIRS, 128, 128), BF16), VMEM((PAIRS, 128, 128), BF16)]
    scratch += [wide, tall, tall, VMEM((TOK, 128), F32), tall, VMEM((18, 8, D), F32)]
    scratch += [wide, tall, wide, VMEM((TOK, 3 * D), BF16)]
    scratch += [row, row, VMEM((8, 128), F32), row, row, row]
    scratch += [wide, wide, VMEM((PAIRS, n, 16, 256), BF16), VMEM((PAIRS, n, 16, 256), BF16)]
    scratch += [VMEM((16, 1024), F32), VMEM((8, 16, 128), F32), VMEM((8, 16, 128), F32)]
    scratch += [
        VMEM((2, 4, 64, 1024), BF16),
        VMEM((4, 64, 1024), BF16),
        VMEM((3, 64, 1024), BF16),
        VMEM((3, 64, 1024), BF16),
        VMEM((64, 1024), F32),
        VMEM((n, 16, 128), BF16),
        VMEM((n, 16, 128), BF16),
        VMEM((2, 16, 128), BF16),
        VMEM((8, 8, 128), F32),
        VMEM((8, 128), F32),
        VMEM((8, 128), F32),
    ]
    for count in (3, n, n, n, n, n, n, n, 2, 2, 2, PAIRS * n, 8, 4, 3, n, 2 * n, 8, n):
        scratch.append(pltpu.SemaphoreType.DMA((2, count)))
    out, grads, small = call(
        functools.partial(layer, n),
        "layer",
        [((TOK, D), BF16), ((2, n, 16, 128), BF16), ((n, 8, 128), F32)],
        scratch,
        (sharp, x, up, gain1, w, wo, factors, gain2, kernels),
        smem=1,
        collective=0,
        away=(2, 4, 5),
    )
    out, gq, gp, conv, scale = call(
        finish,
        "finish",
        [
            ((TOK, D), BF16),
            ((64, 3 * D), F32),
            ((64, D), F32),
            ((3, 3, 2, D), F32),
            ((2, D), F32),
        ],
        [],
        (out, grads, small),
    )
    return out.reshape(1, 2, WIDTH, D), gq, gp, conv.transpose(2, 0, 1, 3), scale


def solution(mesh):
    tokens = P("rep", "sp", None, None)
    in_specs = (tokens, tokens, P(), P(), P(), P(), P(), P(), P())
    out_specs = (tokens, P("rep", None), P("rep", None), P(), P())
    return jax.shard_map(
        functools.partial(shards, mesh.shape["sp"]),
        mesh=mesh,
        in_specs=in_specs,
        out_specs=out_specs,
        check_vma=False,
    )
```

```python
import functools

import jax
import jax.numpy as jnp
from jax import lax
from jax.experimental import pallas as pl
from jax.experimental.pallas import tpu as pltpu
from jax.sharding import PartitionSpec as P

D = 512
HEADS = 8
HEAD_DIM = 64
WIDTH = 256
EPS = 1e-06
F32 = jnp.float32
BF16 = jnp.bfloat16
TOK = 512
PAIRS = 4
VMEM = pltpu.VMEM
MESH_ID = pl.DeviceIdType.MESH
LIMIT = 60 * 1024 * 1024


def dot(a, b, ca, cb):
    return lax.dot_general(a, b, (((ca,), (cb,)), ((), ())), preferred_element_type=F32)


def ds(start, size, multiple=None):
    return pl.ds(pl.multiple_of(start, multiple or size), size)


def norm_parts(u):
    centre = jnp.mean(u, -1, keepdims=True)
    centred = u - centre
    inverse = lax.rsqrt(jnp.mean(centred * centred, -1, keepdims=True) + EPS)
    return centred * inverse, inverse


def norm_back(upstream, gain, normed, inverse):
    scaled = upstream * gain
    return inverse * (
        scaled
        - jnp.mean(scaled, -1, keepdims=True)
        - normed * jnp.mean(scaled * normed, -1, keepdims=True)
    )


def lane_low():
    return lax.broadcasted_iota(jnp.int32, (HEAD_DIM, 128), 1) < HEAD_DIM


def eye_pair():
    lane = lax.broadcasted_iota(jnp.int32, (HEAD_DIM, 128), 1)
    row = lax.broadcasted_iota(jnp.int32, (HEAD_DIM, 128), 0)
    return (lane == row) | (lane == row + HEAD_DIM)


def half_sum(v, low):
    left = jnp.sum(jnp.where(low, v, 0.0), -1, keepdims=True)
    right = jnp.sum(jnp.where(low, 0.0, v), -1, keepdims=True)
    return jnp.where(low, left, right)


def half_max(v, low):
    left = jnp.max(jnp.where(low, v, -jnp.inf), -1, keepdims=True)
    right = jnp.max(jnp.where(low, -jnp.inf, v), -1, keepdims=True)
    return jnp.where(low, left, right)


def pack_pair(full, low):
    return jnp.where(low, full[:HEAD_DIM], full[HEAD_DIM:])


def block_diag(packed, low):
    return jnp.concatenate(
        [jnp.where(low, packed, 0.0), jnp.where(low, 0.0, packed)], axis=0
    ).astype(BF16)


def pair_attention(p, gram_ref, sq_ref, sharp_ref, low, eye):
    gram = gram_ref[8 * p : 8 * p + 8].reshape(HEAD_DIM, 128)
    query_sq = half_sum(jnp.where(eye, sq_ref[p : p + 1, :], 0.0), low)
    query_norm = jnp.sqrt(query_sq + EPS)
    key_norm = jnp.sqrt(sq_ref[PAIRS + p : PAIRS + p + 1, :] + EPS)
    divisor = query_norm * key_norm
    sharp = jnp.where(low, sharp_ref[2 * p], sharp_ref[2 * p + 1])
    scores = sharp * gram / divisor
    exponent = jnp.exp(scores - half_max(scores, low))
    prob = exponent / half_sum(exponent, low)
    return prob, scores, divisor, sharp, query_norm, key_norm


def remote(src, dst, sems, at, **axes):
    return pltpu.make_async_remote_copy(
        src_ref=src,
        dst_ref=dst,
        send_sem=sems.at[0, at],
        recv_sem=sems.at[1, at],
        device_id=axes,
        device_id_type=MESH_ID,
    )


def loop(count, step, first=0, each=1):
    def go(i, _):
        for u in range(each):
            step(i * each + u)
        return 0

    lax.fori_loop(first, count // each, go, 0)


def fold(v):
    return v.reshape(-1, 8, v.shape[-1]).sum(0)


def chunk(j):
    return slice(16 * (j // 8), 16 * (j // 8) + 16), slice(128 * (j % 8), 128 * (j % 8) + 128)


def layer(
    n,
    sharp_ref,
    x_ref,
    up_hbm,
    gain1_ref,
    w_hbm,
    wo_hbm,
    factor_ref,
    gain2_ref,
    kern4_ref,
    out_ref,
    grads_ref,
    small_ref,
    up_ref,
    w_ref,
    wo_ref,
    act1_s,
    mixed_s,
    gmsg,
    ggot,
    gmine,
    gram_s,
    gsq,
    gsqgot,
    gsqmine,
    sq_all,
    sq_s,
    kern_ref,
    up_halo,
    act_halo,
    dh_halo,
    act_edge,
    dh_edge,
    act_s,
    up_s,
    dh_s,
    hid_s,
    dhid_s,
    bd_s,
    bd2_s,
    att_s,
    proj_s,
    normed_s,
    inv_s,
    dact_s,
    acc_s,
    dproj_s,
    dres_s,
    datt_s,
    dmix_s,
    pmsg,
    pgot,
    pmine,
    pg_s,
    smsg,
    sgot,
    gl,
    rb1,
    sb2,
    rb2,
    acc2,
    sb3,
    rb3,
    fin,
    srb,
    ssend,
    sfin,
    s_load,
    s_g1,
    s_g2,
    s_q1,
    s_q2,
    s_p1,
    s_p2,
    s_s1,
    s_up,
    s_act,
    s_dh,
    s_pair,
    s_col,
    s_third,
    s_fourth,
    s_small,
    s_fifth,
):
    me, rep = lax.axis_index("sp"), lax.axis_index("rep")
    reps = 8
    loads = [
        pltpu.make_async_copy(src, dst, s_load.at[0, at])
        for at, (src, dst) in enumerate(((w_hbm, w_ref), (up_hbm, up_ref), (wo_hbm, wo_ref)))
    ]
    for load in loads:
        load.start()
    y, core = rep // 2, lax.rem(rep, 2)
    barrier = pltpu.get_barrier_semaphore()

    def greet(k):
        pl.semaphore_signal(
            barrier, inc=1, device_id={"sp": lax.rem(me + k, n)}, device_id_type=MESH_ID
        )

    loop(n, greet, 1)
    for k in range(1, reps):
        pl.semaphore_signal(
            barrier, inc=1, device_id={"rep": lax.rem(rep + k, reps)}, device_id_type=MESH_ID
        )
    low, eye = lane_low(), eye_pair()
    gain1, gain2 = gain1_ref[...], gain2_ref[...]
    factor0, factor1 = factor_ref[0:1, :], factor_ref[1:2, :]

    def to_above(src, halo, sems):
        return remote(src, halo.at[1], sems, 0, sp=me - 1)

    def to_below(src, halo, sems):
        return remote(src, halo.at[0], sems, 1, sp=me + 1)

    def send_above(src, halo, sems):
        @pl.when(me > 0)
        def _():
            to_above(src, halo, sems).start()

    def send_below(src, halo, sems):
        @pl.when(me < n - 1)
        def _():
            to_below(src, halo, sems).start()

    def halos_in(src, halo, sems):
        @pl.when(me > 0)
        def _():
            to_below(src, halo, sems).wait_recv()

        @pl.when(me == 0)
        def _():
            halo[0] = jnp.zeros((WIDTH, D), BF16)

        @pl.when(me < n - 1)
        def _():
            to_above(src, halo, sems).wait_recv()

        @pl.when(me == n - 1)
        def _():
            halo[1] = jnp.zeros((WIDTH, D), BF16)

    def halos_sent(src, halo, sems):
        @pl.when(me > 0)
        def _():
            to_above(src, halo, sems).wait_send()

        @pl.when(me < n - 1)
        def _():
            to_below(src, halo, sems).wait_send()

    def spread(halo, target):
        def rows(i):
            side, c = i // 4, lax.rem(i, 4)
            target[3 * side, ds(8 + c * 64, 64, 8), :] = halo[side, ds(c * 64, 64), :].astype(F32)

        loop(8, rows)

    class Group:
        def __init__(self, copy, sent, got, sems, at=0):
            self.copy = copy
            near = {"sp": lax.rem(me + 1, n)}
            self.whole = remote(sent, got, sems, at, **near)

    def part_to(msg, got, sems, at=0):
        def copy(k):
            j = lax.rem(me + k, n)
            return remote(msg.at[j], got.at[k], sems, at, sp=j)

        rest = pl.ds(1, n - 1)
        return Group(copy, msg.at[rest], got.at[rest], sems, at)

    def part_from(mine, total, sems, at=0):
        def copy(k):
            return remote(mine, total.at[me], sems, at, sp=lax.rem(me + k, n))

        rest = pl.ds(0, n - 1)
        return Group(copy, total.at[rest], total.at[rest], sems, at)

    def start_all(*groups):
        def start(k):
            for group in groups:
                group.copy(k).start()

        loop(n, start, 1)

    def add_all(group, got, own):
        received(group)
        for k in range(1, n):
            own = own + got[k].astype(F32)
        return own

    def received(group):
        group.whole.wait_recv()

    def sent(group):
        group.whole.wait_send()

    def norm_one(i):
        at = ds(i * 32, 32)
        normed, _ = norm_parts(x_ref[at, :].astype(F32))
        act1_s[at, :] = (normed * gain1).astype(BF16)

    loop(TOK // 32, norm_one, each=4)
    loads[0].wait()

    def mix(i):
        at = ds(i * 256, 256)
        mixed_s[at, :] = dot(act1_s[at, :], w_ref[...], 1, 0).astype(BF16)

    loop(2, mix)
    lines = []
    for p in range(2 * PAIRS):
        sq = jnp.zeros((8, 128), F32)
        for i in range(0, TOK, 64):
            part = mixed_s[i : i + 64, 128 * p : 128 * p + 128].astype(F32)
            sq = sq + fold(part * part)
        lines.append(sq.sum(0, keepdims=True))
    sq = jnp.concatenate(lines, axis=0)
    for p in range(PAIRS):
        query = mixed_s[:, 128 * p : 128 * p + 128]
        key = mixed_s[:, D + 128 * p : D + 128 * p + 128]
        packed = pack_pair(dot(query, key, 0, 0), low)
        for b in range(8):
            gmsg[8 * p + b] = packed[8 * b : 8 * b + 8]
    quarter = lax.broadcasted_iota(jnp.int32, (1, 128), 1) >> 5
    for j in range(n):
        gsq[j] = jnp.where(quarter == j % 4, sq[j // 4 : j // 4 + 1], 0.0)
    pl.semaphore_wait(barrier, n - 1 + reps - 1)
    gram_out, gram_back = part_to(gmsg, ggot, s_g1), part_from(gmine, gram_s, s_g2)
    sq_out, sq_back = part_to(gsq, gsqgot, s_q1), part_from(gsqmine, sq_all, s_q2)
    start_all(gram_out, sq_out)
    up_row = [up_ref.at[pl.ds(0, WIDTH)], up_ref.at[pl.ds(WIDTH, WIDTH)]]

    for at in range(18):
        kern_ref[at : at + 1, :] = kern4_ref[(at // 3) % 3, at % 3, at // 9 : at // 9 + 1, :]
    for ref, count in ((act_s, 4), (up_s, 4), (dh_s, 4), (hid_s, 2)):
        for r in range(count):
            ref[r, 0:8, :] = jnp.zeros((8, D), F32)
            ref[r, 264:272, :] = jnp.zeros((8, D), F32)
    acc_s[...] = jnp.zeros_like(acc_s)

    def upstream_rows(i):
        row, c = i // 4, lax.rem(i, 4)
        up_s[row + 1, ds(8 + c * 64, 64, 8), :] = up_ref[ds(i * 64, 64), :].astype(F32)

    loads[1].wait()
    loop(8, upstream_rows)
    total = add_all(gram_out, ggot, gmsg[me])
    gmine[...] = total
    gram_s[me] = total
    total = add_all(sq_out, gsqgot, gsq[me])
    gsqmine[...] = total
    sq_all[me] = total
    start_all(gram_back, sq_back)
    send_above(up_row[0], up_halo, s_up)
    send_below(up_row[1], up_halo, s_up)
    loads[2].wait()
    received(gram_back)
    received(sq_back)
    for p in range(2 * PAIRS):
        sq_s[p : p + 1, :] = sq_all[4 * p] + sq_all[4 * p + 1] + sq_all[4 * p + 2] + sq_all[4 * p + 3]

    for p in range(PAIRS):
        prob = pair_attention(p, gram_s, sq_s, sharp_ref, low, eye)[0]
        bd_s[p] = block_diag(prob, low)
    for row in range(2):
        at_row = slice(row * WIDTH, row * WIDTH + WIDTH)
        for p in range(PAIRS):
            cols = slice(128 * p, 128 * p + 128)
            value = mixed_s[at_row, 2 * D + 128 * p : 2 * D + 128 * p + 128]
            att_s[at_row, cols] = dot(value, bd_s[p], 1, 1).astype(BF16)
        proj_s[at_row, :] = dot(att_s[at_row, :], wo_ref[...], 1, 0)

        def norm_two(c, row=row):
            at = ds(row * WIDTH + c * 32, 32)
            u = x_ref[at, :].astype(F32) + factor0 * proj_s[at, :]
            normed, inverse = norm_parts(u.astype(BF16).astype(F32))
            act = (normed * gain2).astype(BF16)
            act_edge[row, ds(c * 32, 32), :] = act
            act_s[row + 1, ds(8 + c * 32, 32, 8), :] = act.astype(F32)
            normed_s[at, :] = normed
            inv_s[at, :] = jnp.broadcast_to(inverse, (32, 128))

        loop(WIDTH // 32, norm_two, each=4)
        if row == 0:
            send_above(act_edge.at[0], act_halo, s_act)
        else:
            send_below(act_edge.at[1], act_halo, s_act)

    def taps(which, lanes, i, j):
        at = 9 * which + 3 * i + j
        return kern_ref[at : at + 1, lanes]

    def place(idx):
        return ds((idx // 4) * 128, 128), lax.rem(idx, 4)

    def forth(sums):
        return pltpu.roll(sums[0], 1, 0)[8:72] + sums[1][8:72] + pltpu.roll(sums[2], 79, 0)[8:72]

    def back(sums):
        return pltpu.roll(sums[0], 79, 0)[8:72] + sums[1][8:72] + pltpu.roll(sums[2], 1, 0)[8:72]

    halos_in(up_row[0], up_halo, s_up)
    spread(up_halo, up_s)

    def hidden_grads(idx):
        r = idx // 16
        lanes, c = place(lax.rem(idx, 16))
        win = ds(c * 64, 80, 8)
        near = [up_s[r + 2 - i, win, lanes] for i in range(3)]
        scale = factor_ref[1:2, lanes]
        sums = [sum((taps(1, lanes, i, j) * scale) * near[i] for i in range(3)) for j in range(3)]
        dhid_s[ds(r * WIDTH + c * 64, 64), lanes] = back(sums)

    loop(32, hidden_grads)
    halos_in(act_edge.at[0], act_halo, s_act)
    spread(act_halo, act_s)
    for r in range(2):

        def hidden_row(idx, r=r):
            lanes, c = place(idx)
            win, mid = ds(c * 64, 80, 8), ds(8 + c * 64, 64, 8)
            near = [act_s[r + i, win, lanes] for i in range(3)]
            h = forth([sum(taps(0, lanes, i, j) * near[i] for i in range(3)) for j in range(3)])
            cumul = 0.5 * (1.0 + lax.erf(h * 0.7071067811865476))
            density = jnp.exp(-0.5 * h * h) * 0.3989422804014327
            hid_s[r, mid, lanes] = (h * cumul).astype(BF16).astype(F32)
            d_h = dhid_s[ds(r * WIDTH + c * 64, 64), lanes] * (cumul + h * density)
            dh_s[r + 1, mid, lanes] = d_h
            dh_edge[r, ds(c * 64, 64), lanes] = d_h.astype(BF16)

        loop(16, hidden_row)
        if r == 0:
            send_above(dh_edge.at[0], dh_halo, s_dh)
        else:
            send_below(dh_edge.at[1], dh_halo, s_dh)

    def kernel_grads(idx):
        r = idx // 16
        lanes, c = place(lax.rem(idx, 16))
        win, mid = ds(c * 64, 80, 8), ds(8 + c * 64, 64, 8)
        own = dh_s[r + 1, win, lanes]
        moved = [pltpu.roll(own, 79, 0)[8:72], own[8:72], pltpu.roll(own, 1, 0)[8:72]]
        for i in range(3):
            act = act_s[r + i, mid, lanes]
            for j in range(3):
                acc_s[3 * i + j, :, lanes] += fold(moved[j] * act)
        own = hid_s[r, win, lanes]
        moved = [pltpu.roll(own, 1, 0)[8:72], own[8:72], pltpu.roll(own, 79, 0)[8:72]]
        for i in range(3):
            up = up_s[r + 2 - i, mid, lanes]
            for j in range(3):
                acc_s[9 + 3 * i + j, :, lanes] += fold(moved[j] * up)

    loop(32, kernel_grads)
    halos_in(dh_edge.at[0], dh_halo, s_dh)
    spread(dh_halo, dh_s)

    def act_grads(idx):
        r = idx // 16
        lanes, c = place(lax.rem(idx, 16))
        win = ds(c * 64, 80, 8)
        near = [dh_s[r + 2 - i, win, lanes] for i in range(3)]
        sums = [sum(taps(0, lanes, i, j) * near[i] for i in range(3)) for j in range(3)]
        dact_s[ds(r * WIDTH + c * 64, 64), lanes] = back(sums)

    loop(32, act_grads)

    def residual_rows(step, scale):
        for u in range(4):
            i = 4 * step + u
            row, c = i // 8, lax.rem(i, 8)
            at = ds(i * 32, 32)
            lnb = norm_back(dact_s[at, :], gain2, normed_s[at, :], inv_s[at, 0:1])
            d_res = up_s[row + 1, ds(8 + c * 32, 32, 8), :] + lnb
            dres_s[at, :] = d_res
            dproj_s[at, :] = (factor0 * d_res).astype(BF16)
            scale = scale + fold(proj_s[at, :] * d_res)
        return scale

    scale_one = lax.fori_loop(0, TOK // 128, residual_rows, jnp.zeros((8, D), F32))

    def attended_rows(i):
        at = ds(i * 256, 256)
        datt_s[at, :] = dot(dproj_s[at, :], wo_ref[...], 1, 1).astype(BF16)

    loop(2, attended_rows)
    for p in range(PAIRS):
        cols = slice(128 * p, 128 * p + 128)
        value = mixed_s[:, 2 * D + 128 * p : 2 * D + 128 * p + 128]
        packed = pack_pair(dot(datt_s[:, cols], value, 0, 0), low)
        for b in range(8):
            pmsg[8 * p + b] = packed[8 * b : 8 * b + 8]
    prob_out, prob_back = part_to(pmsg, pgot, s_p1), part_from(pmine, pg_s, s_p2)
    start_all(prob_out)
    lines = [acc_s[m].sum(0, keepdims=True) for m in range(18)]
    scale_two = sum(lines[9 + m] * kern_ref[9 + m : 10 + m, :] for m in range(9))
    lines = lines[:9] + [line * factor1 for line in lines[9:]]
    lines += [scale_one.sum(0, keepdims=True), scale_two]
    smsg[...] = jnp.zeros_like(smsg)
    for at in range(80):
        v, b = at // 4, at % 4
        smsg[at // 3, at % 3 : at % 3 + 1, :] = lines[v][:, 128 * b : 128 * b + 128]
    small_out = part_to(smsg, sgot, s_s1)
    start_all(small_out)

    def grads(half, block, left, right):
        for side in range(2):
            g = dot(left[:, 256 * side : 256 * side + 256], right, 0, 0).astype(BF16)
            for r in range(4):
                at = 4 * side + r
                gl[half, at % 2, at // 2, :, 512 * block : 512 * block + 512] = g[
                    64 * r : 64 * r + 64
                ]

    def pair_copy(half, k):
        there = lax.rem(y + 1 + k, 4)
        return remote(
            gl.at[half, 1 - core, there],
            rb1.at[half, k],
            s_pair,
            4 * half + k,
            rep=2 * y + 1 - core,
        )

    def column_copy(half, k):
        there = lax.rem(y + 1 + k, 4)
        return remote(
            sb2.at[half, k], rb2.at[half, k], s_col, 3 * half + k, rep=2 * there + core
        )

    def pair_start(half):
        for k in range(4):
            pair_copy(half, k).start()

    def pair_finish(half):
        for k in range(3):
            there = lax.rem(y + 1 + k, 4)
            pair_copy(half, k).wait_recv()

            def add(i, k=k, there=there):
                at = ds(i * 16, 16)
                sb2[half, k, at, :] = (
                    gl[half, core, there, at, :].astype(F32) + rb1[half, k, at, :].astype(F32)
                ).astype(BF16)

            loop(4, add)
            column_copy(half, k).start()
        pair_copy(half, 3).wait_recv()

        def own(i):
            at = ds(i * 16, 16)
            acc2[half, at, :] = gl[half, core, y, at, :].astype(F32) + rb1[half, 3, at, :].astype(
                F32
            )

        loop(4, own)

    third = [part_to(sb3.at[half], rb3.at[half], s_third, half) for half in range(2)]
    fourth = [
        part_from(fin.at[half], grads_ref.at[half], s_fourth, half) for half in range(2)
    ]

    def column_finish(half):
        for k in range(3):
            column_copy(half, k).wait_recv()
        for j in range(n):
            rows, cols = chunk(j)
            total = acc2[half, rows, cols]
            for k in range(3):
                total = total + rb2[half, k, rows, cols].astype(F32)
            sb3[half, j] = total.astype(BF16)
        start_all(third[half])

    def third_finish(half):
        total = add_all(third[half], rb3.at[half], sb3[half, me].astype(F32)).astype(BF16)
        fin[half] = total
        grads_ref[half, me] = total
        start_all(fourth[half])

    for p in range(PAIRS):
        cols = slice(128 * p, 128 * p + 128)
        for i in range(0, TOK, 256):
            dmix_s[i : i + 256, 2 * D + 128 * p : 2 * D + 128 * p + 128] = dot(
                datt_s[i : i + 256, cols], bd_s[p], 1, 0
            ).astype(BF16)
    grads(1, 0, act1_s, dmix_s[:, 2 * D :])
    grads(1, 1, att_s, dproj_s[...])
    pair_start(1)
    pair_finish(1)
    total = add_all(prob_out, pgot, pmsg[me])
    pmine[...] = total
    start_all(prob_back)
    pg_s[me] = total
    total = add_all(small_out, sgot, smsg[me])
    ssend[...] = total
    srb[rep] = total

    def small_copy(k):
        return remote(ssend, srb.at[rep], s_small, 0, rep=lax.rem(rep + k, reps))

    smalls = srb.at[pl.ds(0, reps - 1)]
    small_all = remote(smalls, smalls, s_small, 0, rep=lax.rem(rep + 1, reps))

    for k in range(1, reps):
        small_copy(k).start()
    received(prob_back)

    for p in range(PAIRS):
        prob, scores, divisor, sharp, query_norm, key_norm = pair_attention(
            p, gram_s, sq_s, sharp_ref, low, eye
        )
        pg = pg_s[8 * p : 8 * p + 8].reshape(HEAD_DIM, 128)
        logit = prob * (pg - half_sum(prob * pg, low))
        bd2_s[p] = block_diag(logit * sharp / divisor, low)
        weighted = logit * scores
        d_qsq = -half_sum(weighted, low) / (2.0 * query_norm * query_norm)
        d_qsq = 2.0 * jnp.sum(jnp.where(eye, d_qsq, 0.0), 0, keepdims=True)
        d_ksq = -2.0 * jnp.sum(weighted, 0, keepdims=True) / (2.0 * key_norm * key_norm)
        qc = slice(128 * p, 128 * p + 128)
        kc = slice(D + 128 * p, D + 128 * p + 128)
        for i in range(0, TOK, 256):
            at = slice(i, i + 256)
            query, key = mixed_s[at, qc], mixed_s[at, kc]
            dmix_s[at, qc] = (dot(key, bd2_s[p], 1, 1) + d_qsq * query.astype(F32)).astype(BF16)
            dmix_s[at, kc] = (dot(query, bd2_s[p], 1, 0) + d_ksq * key.astype(F32)).astype(BF16)

    def inputs(i):
        at = ds(i * 256, 256)
        dact_s[at, :] = dot(dmix_s[at, :], w_ref[...], 1, 1)

    grads(0, 0, act1_s, dmix_s[:, :D])
    grads(0, 1, act1_s, dmix_s[:, D : 2 * D])
    pair_start(0)
    column_finish(1)
    pair_finish(0)
    loop(2, inputs)

    def input_rows(i):
        at = ds(i * 32, 32)
        normed, inverse = norm_parts(x_ref[at, :].astype(F32))
        lnb = norm_back(dact_s[at, :], gain1, normed, inverse)
        out_ref[at, :] = (dres_s[at, :] + lnb).astype(BF16)

    loop(TOK // 32, input_rows, each=4)
    column_finish(0)
    third_finish(1)
    small_all.wait_recv()
    total = srb[0]
    for k in range(1, reps):
        total = total + srb[k]
    sfin[...] = total
    small_ref[me] = total
    fifth = part_from(sfin, small_ref, s_fifth)
    start_all(fifth)
    third_finish(0)

    for copy in (gram_out, gram_back, sq_out, sq_back, prob_out, prob_back, small_out, third[0], third[1]):
        sent(copy)
    for src, halo, sems in (
        (up_row[0], up_halo, s_up),
        (act_edge.at[0], act_halo, s_act),
        (dh_edge.at[0], dh_halo, s_dh),
    ):
        halos_sent(src, halo, sems)
    small_all.wait_send()
    for half in range(2):
        for k in range(4):
            pair_copy(half, k).wait_send()
        for k in range(3):
            column_copy(half, k).wait_send()
    for copy in (fourth[1], fifth, fourth[0]):
        received(copy)
        sent(copy)


def finish(out_in, grads_ref, small_ref, out_ref, gq_ref, gp_ref, conv_ref, scale_ref):
    out_ref[...] = out_in[...]
    for j in range(32):
        rows, cols = chunk(j)
        gq_ref[rows, cols] = grads_ref[0, j].astype(F32)
        if cols.start < D:
            gq_ref[rows, 2 * D + cols.start : 2 * D + cols.stop] = grads_ref[1, j].astype(F32)
        else:
            gp_ref[rows, cols.start - D : cols.stop - D] = grads_ref[1, j].astype(F32)
    for at in range(80):
        v, b = at // 4, at % 4
        line = small_ref[at // 3, at % 3 : at % 3 + 1, :]
        lanes = slice(128 * b, 128 * b + 128)
        if v < 18:
            conv_ref[(v // 3) % 3, v % 3, v // 9 : v // 9 + 1, lanes] = line
        else:
            scale_ref[v - 18 : v - 17, lanes] = line


def call(body, name, outs, scratch, args, smem=0, collective=None, away=()):
    params = dict(vmem_limit_bytes=LIMIT)
    if collective is not None:
        params.update(collective_id=collective, has_side_effects=True)
    specs = [pl.BlockSpec(memory_space=pltpu.SMEM)] * smem
    specs += [
        pl.BlockSpec(memory_space=pl.ANY if at in away else VMEM) for at in range(smem, len(args))
    ]
    return pl.pallas_call(
        body,
        name=name,
        out_shape=[jax.ShapeDtypeStruct(s, t) for s, t in outs],
        in_specs=specs,
        out_specs=[pl.BlockSpec(memory_space=VMEM)] * len(outs),
        scratch_shapes=scratch,
        compiler_params=pltpu.CompilerParams(**params),
    )(*args)


def shards(n, x, up, gain1, w, sharp, wo, factors, gain2, kernels):
    x = x.reshape(TOK, D)
    up = up.reshape(TOK, D)
    gain1, gain2 = gain1.reshape(1, D), gain2.reshape(1, D)
    kernels = kernels.transpose(1, 2, 0, 3)
    row = VMEM((n, 8, 128), F32)
    edge = VMEM((2, WIDTH, D), BF16)
    wide, tall = VMEM((TOK, D), BF16), VMEM((TOK, D), F32)
    scratch = [wide, VMEM((D, 3 * D), BF16), wide, wide, VMEM((TOK, 3 * D), BF16)]
    scratch += [row, row, VMEM((8, 128), F32), row]
    scratch += [VMEM((n, 1, 128), F32), VMEM((n, 1, 128), F32), VMEM((1, 128), F32)]
    scratch += [VMEM((n, 1, 128), F32), VMEM((8, 128), F32), VMEM((18, D), F32)]
    scratch += [edge] * 5
    scratch += [VMEM((count, 272, D), F32) for count in (4, 4, 4, 2)]
    scratch += [tall, VMEM((PAIRS, 128, 128), BF16), VMEM((PAIRS, 128, 128), BF16)]
    scratch += [wide, tall, tall, VMEM((TOK, 128), F32), tall, VMEM((18, 8, D), F32)]
    scratch += [wide, tall, wide, VMEM((TOK, 3 * D), BF16)]
    scratch += [row, row, VMEM((8, 128), F32), row, row, row]
    scratch += [
        VMEM((2, 2, 4, 64, 1024), BF16),
        VMEM((2, 4, 64, 1024), BF16),
        VMEM((2, 3, 64, 1024), BF16),
        VMEM((2, 3, 64, 1024), BF16),
        VMEM((2, 64, 1024), F32),
        VMEM((2, n, 16, 128), BF16),
        VMEM((2, n, 16, 128), BF16),
        VMEM((2, 16, 128), BF16),
        VMEM((8, 8, 128), F32),
        VMEM((8, 128), F32),
        VMEM((8, 128), F32),
    ]
    for count in (3, 1, 1, 1, 1, 1, 1, 1, 2, 2, 2, 8, 6, 2, 2, 1, 1):
        scratch.append(pltpu.SemaphoreType.DMA((2, count)))
    out, grads, small = call(
        functools.partial(layer, n),
        "layer",
        [((TOK, D), BF16), ((2, n, 16, 128), BF16), ((n, 8, 128), F32)],
        scratch,
        (sharp, x, up, gain1, w, wo, factors, gain2, kernels),
        smem=1,
        collective=0,
        away=(2, 4, 5),
    )
    out, gq, gp, conv, scale = call(
        finish,
        "finish",
        [
            ((TOK, D), BF16),
            ((64, 3 * D), F32),
            ((64, D), F32),
            ((3, 3, 2, D), F32),
            ((2, D), F32),
        ],
        [],
        (out, grads, small),
    )
    return out.reshape(1, 2, WIDTH, D), gq, gp, conv.transpose(2, 0, 1, 3), scale


def solution(mesh):
    tokens = P("rep", "sp", None, None)
    in_specs = (tokens, tokens, P(), P(), P(), P(), P(), P(), P())
    out_specs = (tokens, P("rep", None), P("rep", None), P(), P())
    return jax.shard_map(
        functools.partial(shards, mesh.shape["sp"]),
        mesh=mesh,
        in_specs=in_specs,
        out_specs=out_specs,
        check_vma=False,
    )
```

```python
import functools

import jax
import jax.numpy as jnp
from jax import lax
from jax.experimental import pallas as pl
from jax.experimental.pallas import tpu as pltpu
from jax.sharding import PartitionSpec as P

D = 512
HEADS = 8
HEAD_DIM = 64
WIDTH = 256
EPS = 1e-06
F32 = jnp.float32
BF16 = jnp.bfloat16
TOK = 512
PAIRS = 4
VMEM = pltpu.VMEM
MESH_ID = pl.DeviceIdType.MESH
LIMIT = 60 * 1024 * 1024


def dot(a, b, ca, cb):
    return lax.dot_general(a, b, (((ca,), (cb,)), ((), ())), preferred_element_type=F32)


def ds(start, size, multiple=None):
    return pl.ds(pl.multiple_of(start, multiple or size), size)


def norm_parts(u):
    centre = jnp.mean(u, -1, keepdims=True)
    centred = u - centre
    inverse = lax.rsqrt(jnp.mean(centred * centred, -1, keepdims=True) + EPS)
    return centred * inverse, inverse


def norm_back(upstream, gain, normed, inverse):
    scaled = upstream * gain
    return inverse * (
        scaled
        - jnp.mean(scaled, -1, keepdims=True)
        - normed * jnp.mean(scaled * normed, -1, keepdims=True)
    )


def lane_low():
    return lax.broadcasted_iota(jnp.int32, (HEAD_DIM, 128), 1) < HEAD_DIM


def eye_pair():
    lane = lax.broadcasted_iota(jnp.int32, (HEAD_DIM, 128), 1)
    row = lax.broadcasted_iota(jnp.int32, (HEAD_DIM, 128), 0)
    return (lane == row) | (lane == row + HEAD_DIM)


def half_sum(v, low):
    left = jnp.sum(jnp.where(low, v, 0.0), -1, keepdims=True)
    right = jnp.sum(jnp.where(low, 0.0, v), -1, keepdims=True)
    return jnp.where(low, left, right)


def half_max(v, low):
    left = jnp.max(jnp.where(low, v, -jnp.inf), -1, keepdims=True)
    right = jnp.max(jnp.where(low, -jnp.inf, v), -1, keepdims=True)
    return jnp.where(low, left, right)


def pack_pair(full, low):
    return jnp.where(low, full[:HEAD_DIM], full[HEAD_DIM:])


def block_diag(packed, low):
    return jnp.concatenate(
        [jnp.where(low, packed, 0.0), jnp.where(low, 0.0, packed)], axis=0
    ).astype(BF16)


def pair_attention(p, gram_ref, sq_ref, sharp_ref, low, eye):
    gram = gram_ref[8 * p : 8 * p + 8].reshape(HEAD_DIM, 128)
    query_sq = half_sum(jnp.where(eye, sq_ref[p : p + 1, :], 0.0), low)
    query_norm = jnp.sqrt(query_sq + EPS)
    key_norm = jnp.sqrt(sq_ref[PAIRS + p : PAIRS + p + 1, :] + EPS)
    divisor = query_norm * key_norm
    sharp = jnp.where(low, sharp_ref[2 * p], sharp_ref[2 * p + 1])
    scores = sharp * gram / divisor
    exponent = jnp.exp(scores - half_max(scores, low))
    prob = exponent / half_sum(exponent, low)
    return prob, scores, divisor, sharp, query_norm, key_norm


def remote(src, dst, sems, at, **axes):
    return pltpu.make_async_remote_copy(
        src_ref=src,
        dst_ref=dst,
        send_sem=sems.at[0, at],
        recv_sem=sems.at[1, at],
        device_id=axes,
        device_id_type=MESH_ID,
    )


def loop(count, step, first=0, each=1):
    def go(i, _):
        for u in range(each):
            step(i * each + u)
        return 0

    lax.fori_loop(first, count // each, go, 0)


def fold(v):
    return v.reshape(-1, 8, v.shape[-1]).sum(0)


def chunk(j):
    return slice(16 * (j // 8), 16 * (j // 8) + 16), slice(128 * (j % 8), 128 * (j % 8) + 128)


def layer(
    n,
    sharp_hbm,
    x_hbm,
    up_hbm,
    gain1_hbm,
    w_hbm,
    wo_hbm,
    factor_hbm,
    gain2_hbm,
    kern4_hbm,
    out_ref,
    grads_ref,
    small_ref,
    sharp_ref,
    x_ref,
    gain1_ref,
    factor_ref,
    gain2_ref,
    kern4_ref,
    up_ref,
    w_ref,
    wo_ref,
    act1_s,
    mixed_s,
    gmsg,
    ggot,
    gmine,
    gram_s,
    gsq,
    gsqgot,
    gsqmine,
    sq_all,
    sq_s,
    kern_ref,
    up_halo,
    act_halo,
    dh_halo,
    act_edge,
    dh_edge,
    act_s,
    up_s,
    dh_s,
    hid_s,
    dhid_s,
    bd_s,
    bd2_s,
    att_s,
    proj_s,
    normed_s,
    inv_s,
    dact_s,
    acc_s,
    dproj_s,
    dres_s,
    datt_s,
    dmix_s,
    pmsg,
    pgot,
    pmine,
    pg_s,
    smsg,
    sgot,
    gl,
    rb1,
    sb2,
    rb2,
    acc2,
    sb3,
    rb3,
    fin,
    srb,
    ssend,
    sfin,
    s_load,
    s_g1,
    s_g2,
    s_q1,
    s_q2,
    s_p1,
    s_p2,
    s_s1,
    s_up,
    s_act,
    s_dh,
    s_pair,
    s_col,
    s_third,
    s_fourth,
    s_small,
    s_fifth,
):
    me, rep = lax.axis_index("sp"), lax.axis_index("rep")
    reps = 8
    moves = (
        (x_hbm, x_ref),
        (gain1_hbm, gain1_ref),
        (w_hbm, w_ref),
        (up_hbm, up_ref),
        (wo_hbm, wo_ref),
        (sharp_hbm, sharp_ref),
        (factor_hbm, factor_ref),
        (gain2_hbm, gain2_ref),
        (kern4_hbm, kern4_ref),
    )
    loads = [
        pltpu.make_async_copy(src, dst, s_load.at[0, at]) for at, (src, dst) in enumerate(moves)
    ]
    y, core = rep // 2, lax.rem(rep, 2)
    barrier = pltpu.get_barrier_semaphore()
    loads[0].start()
    loads[1].start()

    def greet(k):
        pl.semaphore_signal(
            barrier, inc=1, device_id={"sp": lax.rem(me + k, n)}, device_id_type=MESH_ID
        )

    loop(n, greet, 1)
    for k in range(1, reps):
        pl.semaphore_signal(
            barrier, inc=1, device_id={"rep": lax.rem(rep + k, reps)}, device_id_type=MESH_ID
        )
    for load in loads[2:]:
        load.start()
    low, eye = lane_low(), eye_pair()

    def to_above(src, halo, sems):
        return remote(src, halo.at[1], sems, 0, sp=me - 1)

    def to_below(src, halo, sems):
        return remote(src, halo.at[0], sems, 1, sp=me + 1)

    def send_above(src, halo, sems):
        @pl.when(me > 0)
        def _():
            to_above(src, halo, sems).start()

    def send_below(src, halo, sems):
        @pl.when(me < n - 1)
        def _():
            to_below(src, halo, sems).start()

    def halos_in(src, halo, sems):
        @pl.when(me > 0)
        def _():
            to_below(src, halo, sems).wait_recv()

        @pl.when(me == 0)
        def _():
            halo[0] = jnp.zeros((WIDTH, D), BF16)

        @pl.when(me < n - 1)
        def _():
            to_above(src, halo, sems).wait_recv()

        @pl.when(me == n - 1)
        def _():
            halo[1] = jnp.zeros((WIDTH, D), BF16)

    def halos_sent(src, halo, sems):
        @pl.when(me > 0)
        def _():
            to_above(src, halo, sems).wait_send()

        @pl.when(me < n - 1)
        def _():
            to_below(src, halo, sems).wait_send()

    def spread(halo, target):
        def rows(i):
            side, c = i // 4, lax.rem(i, 4)
            target[3 * side, ds(8 + c * 64, 64, 8), :] = halo[side, ds(c * 64, 64), :].astype(F32)

        loop(8, rows)

    class Group:
        def __init__(self, copy, sent, got, sems, at=0):
            self.copy = copy
            near = {"sp": lax.rem(me + 1, n)}
            self.whole = remote(sent, got, sems, at, **near)

    def part_to(msg, got, sems, at=0):
        def copy(k):
            j = lax.rem(me + k, n)
            return remote(msg.at[j], got.at[k], sems, at, sp=j)

        rest = pl.ds(1, n - 1)
        return Group(copy, msg.at[rest], got.at[rest], sems, at)

    def part_from(mine, total, sems, at=0):
        def copy(k):
            return remote(mine, total.at[me], sems, at, sp=lax.rem(me + k, n))

        rest = pl.ds(0, n - 1)
        return Group(copy, total.at[rest], total.at[rest], sems, at)

    def start_all(*groups):
        def start(t):
            k = n // 2 + (t // 2) * (1 - 2 * lax.rem(t, 2))
            for group in groups:
                group.copy(k).start()

        loop(n, start, 1)

    def add_all(group, got, own):
        received(group)
        for k in range(1, n):
            own = own + got[k].astype(F32)
        return own

    def received(group):
        group.whole.wait_recv()

    def sent(group):
        group.whole.wait_send()

    loads[0].wait()
    loads[1].wait()
    gain1 = gain1_ref[...]

    def norm_one(i):
        at = ds(i * 32, 32)
        normed, _ = norm_parts(x_ref[at, :].astype(F32))
        act1_s[at, :] = (normed * gain1).astype(BF16)

    loop(TOK // 32, norm_one, each=4)
    loads[2].wait()

    def mix(i):
        at = ds(i * 256, 256)
        mixed_s[at, :] = dot(act1_s[at, :], w_ref[...], 1, 0).astype(BF16)

    loop(2, mix)
    lines = []
    for p in range(2 * PAIRS):
        sq = jnp.zeros((8, 128), F32)
        for i in range(0, TOK, 64):
            part = mixed_s[i : i + 64, 128 * p : 128 * p + 128].astype(F32)
            sq = sq + fold(part * part)
        lines.append(sq.sum(0, keepdims=True))
    sq = jnp.concatenate(lines, axis=0)
    for p in range(PAIRS):
        query = mixed_s[:, 128 * p : 128 * p + 128]
        key = mixed_s[:, D + 128 * p : D + 128 * p + 128]
        packed = pack_pair(dot(query, key, 0, 0), low)
        for b in range(8):
            gmsg[8 * p + b] = packed[8 * b : 8 * b + 8]
    quarter = lax.broadcasted_iota(jnp.int32, (1, 128), 1) >> 5
    for j in range(n):
        gsq[j] = jnp.where(quarter == j % 4, sq[j // 4 : j // 4 + 1], 0.0)
    pl.semaphore_wait(barrier, n - 1 + reps - 1)
    gram_out, gram_back = part_to(gmsg, ggot, s_g1), part_from(gmine, gram_s, s_g2)
    sq_out, sq_back = part_to(gsq, gsqgot, s_q1), part_from(gsqmine, sq_all, s_q2)
    start_all(gram_out, sq_out)
    up_row = [up_ref.at[pl.ds(0, WIDTH)], up_ref.at[pl.ds(WIDTH, WIDTH)]]

    for load in loads[3:]:
        load.wait()
    gain2 = gain2_ref[...]
    factor0, factor1 = factor_ref[0:1, :], factor_ref[1:2, :]
    for at in range(18):
        kern_ref[at : at + 1, :] = kern4_ref[(at // 3) % 3, at % 3, at // 9 : at // 9 + 1, :]
    for ref, count in ((act_s, 4), (up_s, 4), (dh_s, 4), (hid_s, 2)):
        for r in range(count):
            ref[r, 0:8, :] = jnp.zeros((8, D), F32)
            ref[r, 264:272, :] = jnp.zeros((8, D), F32)
    acc_s[...] = jnp.zeros_like(acc_s)

    def upstream_rows(i):
        row, c = i // 4, lax.rem(i, 4)
        up_s[row + 1, ds(8 + c * 64, 64, 8), :] = up_ref[ds(i * 64, 64), :].astype(F32)

    loop(8, upstream_rows)
    total = add_all(gram_out, ggot, gmsg[me])
    gmine[...] = total
    gram_s[me] = total
    total = add_all(sq_out, gsqgot, gsq[me])
    gsqmine[...] = total
    sq_all[me] = total
    start_all(gram_back, sq_back)
    send_above(up_row[0], up_halo, s_up)
    send_below(up_row[1], up_halo, s_up)
    received(gram_back)
    received(sq_back)
    for p in range(2 * PAIRS):
        sq_s[p : p + 1, :] = sq_all[4 * p] + sq_all[4 * p + 1] + sq_all[4 * p + 2] + sq_all[4 * p + 3]

    for p in range(PAIRS):
        prob = pair_attention(p, gram_s, sq_s, sharp_ref, low, eye)[0]
        bd_s[p] = block_diag(prob, low)
    for row in range(2):
        at_row = slice(row * WIDTH, row * WIDTH + WIDTH)
        for p in range(PAIRS):
            cols = slice(128 * p, 128 * p + 128)
            value = mixed_s[at_row, 2 * D + 128 * p : 2 * D + 128 * p + 128]
            att_s[at_row, cols] = dot(value, bd_s[p], 1, 1).astype(BF16)
        proj_s[at_row, :] = dot(att_s[at_row, :], wo_ref[...], 1, 0)

        def norm_two(c, row=row):
            at = ds(row * WIDTH + c * 32, 32)
            u = x_ref[at, :].astype(F32) + factor0 * proj_s[at, :]
            normed, inverse = norm_parts(u.astype(BF16).astype(F32))
            act = (normed * gain2).astype(BF16)
            act_edge[row, ds(c * 32, 32), :] = act
            act_s[row + 1, ds(8 + c * 32, 32, 8), :] = act.astype(F32)
            normed_s[at, :] = normed
            inv_s[at, :] = jnp.broadcast_to(inverse, (32, 128))

        loop(WIDTH // 32, norm_two, each=4)
        if row == 0:
            send_above(act_edge.at[0], act_halo, s_act)
        else:
            send_below(act_edge.at[1], act_halo, s_act)

    def taps(which, lanes, i, j):
        at = 9 * which + 3 * i + j
        return kern_ref[at : at + 1, lanes]

    def place(idx):
        return ds((idx // 4) * 128, 128), lax.rem(idx, 4)

    def forth(sums):
        return pltpu.roll(sums[0], 1, 0)[8:72] + sums[1][8:72] + pltpu.roll(sums[2], 79, 0)[8:72]

    def back(sums):
        return pltpu.roll(sums[0], 79, 0)[8:72] + sums[1][8:72] + pltpu.roll(sums[2], 1, 0)[8:72]

    halos_in(up_row[0], up_halo, s_up)
    spread(up_halo, up_s)

    def hidden_grads(idx):
        r = idx // 16
        lanes, c = place(lax.rem(idx, 16))
        win = ds(c * 64, 80, 8)
        near = [up_s[r + 2 - i, win, lanes] for i in range(3)]
        scale = factor_ref[1:2, lanes]
        sums = [sum((taps(1, lanes, i, j) * scale) * near[i] for i in range(3)) for j in range(3)]
        dhid_s[ds(r * WIDTH + c * 64, 64), lanes] = back(sums)

    loop(32, hidden_grads)

    def own_part(target, source, rows, join):
        for r in range(2):

            def go(idx, r=r):
                lanes, c = place(idx)
                win = ds(c * 64, 80, 8)
                near = {i: source[rows(r, i), win, lanes] for i in range(3) if rows(r, i) in (1, 2)}
                target[ds(r * WIDTH + c * 64, 64), lanes] = join(
                    [sum(taps(0, lanes, i, j) * near[i] for i in near) for j in range(3)]
                )

            loop(16, go)

    def halo_part(source, row, i, win, lanes, join):
        near = source[row, win, lanes]
        return join([taps(0, lanes, i, j) * near for j in range(3)])

    own_part(dact_s, act_s, lambda r, i: r + i, forth)
    halos_in(act_edge.at[0], act_halo, s_act)
    spread(act_halo, act_s)
    for r in range(2):

        def hidden_row(idx, r=r):
            lanes, c = place(idx)
            win, mid = ds(c * 64, 80, 8), ds(8 + c * 64, 64, 8)
            h = dact_s[ds(r * WIDTH + c * 64, 64), lanes] + halo_part(
                act_s, 3 * r, 2 * r, win, lanes, forth
            )
            cumul = 0.5 * (1.0 + lax.erf(h * 0.7071067811865476))
            density = jnp.exp(-0.5 * h * h) * 0.3989422804014327
            hid_s[r, mid, lanes] = (h * cumul).astype(BF16).astype(F32)
            d_h = dhid_s[ds(r * WIDTH + c * 64, 64), lanes] * (cumul + h * density)
            dh_s[r + 1, mid, lanes] = d_h
            dh_edge[r, ds(c * 64, 64), lanes] = d_h.astype(BF16)

        loop(16, hidden_row)
        if r == 0:
            send_above(dh_edge.at[0], dh_halo, s_dh)
        else:
            send_below(dh_edge.at[1], dh_halo, s_dh)

    def kernel_grads(idx):
        r = idx // 16
        lanes, c = place(lax.rem(idx, 16))
        win, mid = ds(c * 64, 80, 8), ds(8 + c * 64, 64, 8)
        own = dh_s[r + 1, win, lanes]
        moved = [pltpu.roll(own, 79, 0)[8:72], own[8:72], pltpu.roll(own, 1, 0)[8:72]]
        for i in range(3):
            act = act_s[r + i, mid, lanes]
            for j in range(3):
                acc_s[3 * i + j, :, lanes] += fold(moved[j] * act)
        own = hid_s[r, win, lanes]
        moved = [pltpu.roll(own, 1, 0)[8:72], own[8:72], pltpu.roll(own, 79, 0)[8:72]]
        for i in range(3):
            up = up_s[r + 2 - i, mid, lanes]
            for j in range(3):
                acc_s[9 + 3 * i + j, :, lanes] += fold(moved[j] * up)

    loop(32, kernel_grads)
    own_part(dact_s, dh_s, lambda r, i: r + 2 - i, back)
    halos_in(dh_edge.at[0], dh_halo, s_dh)
    spread(dh_halo, dh_s)

    for r in range(2):

        def act_grads(idx, r=r):
            lanes, c = place(idx)
            win, at = ds(c * 64, 80, 8), ds(r * WIDTH + c * 64, 64)
            dact_s[at, lanes] = dact_s[at, lanes] + halo_part(
                dh_s, 3 * r, 2 - 2 * r, win, lanes, back
            )

        loop(16, act_grads)

    def residual_rows(step, scale):
        for u in range(4):
            i = 4 * step + u
            row, c = i // 8, lax.rem(i, 8)
            at = ds(i * 32, 32)
            lnb = norm_back(dact_s[at, :], gain2, normed_s[at, :], inv_s[at, 0:1])
            d_res = up_s[row + 1, ds(8 + c * 32, 32, 8), :] + lnb
            dres_s[at, :] = d_res
            dproj_s[at, :] = (factor0 * d_res).astype(BF16)
            scale = scale + fold(proj_s[at, :] * d_res)
        return scale

    scale_one = lax.fori_loop(0, TOK // 128, residual_rows, jnp.zeros((8, D), F32))

    def attended_rows(i):
        at = ds(i * 256, 256)
        datt_s[at, :] = dot(dproj_s[at, :], wo_ref[...], 1, 1).astype(BF16)

    loop(2, attended_rows)
    for p in range(PAIRS):
        cols = slice(128 * p, 128 * p + 128)
        value = mixed_s[:, 2 * D + 128 * p : 2 * D + 128 * p + 128]
        packed = pack_pair(dot(datt_s[:, cols], value, 0, 0), low)
        for b in range(8):
            pmsg[8 * p + b] = packed[8 * b : 8 * b + 8]
    prob_out, prob_back = part_to(pmsg, pgot, s_p1), part_from(pmine, pg_s, s_p2)
    start_all(prob_out)
    lines = [acc_s[m].sum(0, keepdims=True) for m in range(18)]
    scale_two = sum(lines[9 + m] * kern_ref[9 + m : 10 + m, :] for m in range(9))
    lines = lines[:9] + [line * factor1 for line in lines[9:]]
    lines += [scale_one.sum(0, keepdims=True), scale_two]
    smsg[...] = jnp.zeros_like(smsg)
    for at in range(80):
        v, b = at // 4, at % 4
        smsg[at // 3, at % 3 : at % 3 + 1, :] = lines[v][:, 128 * b : 128 * b + 128]
    small_out = part_to(smsg, sgot, s_s1)
    start_all(small_out)

    def grads(half, block, left, right):
        for side in range(2):
            g = dot(left[:, 256 * side : 256 * side + 256], right, 0, 0).astype(BF16)
            for r in range(4):
                at = 4 * side + r
                gl[half, at % 2, at // 2, :, 512 * block : 512 * block + 512] = g[
                    64 * r : 64 * r + 64
                ]

    def pair_copy(half, k):
        there = lax.rem(y + 1 + k, 4)
        return remote(
            gl.at[half, 1 - core, there],
            rb1.at[half, k],
            s_pair,
            4 * half + k,
            rep=2 * y + 1 - core,
        )

    def column_copy(half, k):
        there = lax.rem(y + 1 + k, 4)
        return remote(
            sb2.at[half, k], rb2.at[half, k], s_col, 3 * half + k, rep=2 * there + core
        )

    def pair_start(half):
        for k in range(4):
            pair_copy(half, k).start()

    def pair_finish(half):
        for k in range(3):
            there = lax.rem(y + 1 + k, 4)
            pair_copy(half, k).wait_recv()

            def add(i, k=k, there=there):
                at = ds(i * 16, 16)
                sb2[half, k, at, :] = (
                    gl[half, core, there, at, :].astype(F32) + rb1[half, k, at, :].astype(F32)
                ).astype(BF16)

            loop(4, add)
            column_copy(half, k).start()
        pair_copy(half, 3).wait_recv()

        def own(i):
            at = ds(i * 16, 16)
            acc2[half, at, :] = gl[half, core, y, at, :].astype(F32) + rb1[half, 3, at, :].astype(
                F32
            )

        loop(4, own)

    third = [part_to(sb3.at[half], rb3.at[half], s_third, half) for half in range(2)]
    fourth = [
        part_from(fin.at[half], grads_ref.at[half], s_fourth, half) for half in range(2)
    ]

    def column_finish(half):
        for k in range(3):
            column_copy(half, k).wait_recv()
        for j in range(n):
            rows, cols = chunk(j)
            total = acc2[half, rows, cols]
            for k in range(3):
                total = total + rb2[half, k, rows, cols].astype(F32)
            sb3[half, j] = total.astype(BF16)
        start_all(third[half])

    def third_finish(half):
        total = add_all(third[half], rb3.at[half], sb3[half, me].astype(F32)).astype(BF16)
        fin[half] = total
        grads_ref[half, me] = total
        start_all(fourth[half])

    for p in range(PAIRS):
        cols = slice(128 * p, 128 * p + 128)
        for i in range(0, TOK, 256):
            dmix_s[i : i + 256, 2 * D + 128 * p : 2 * D + 128 * p + 128] = dot(
                datt_s[i : i + 256, cols], bd_s[p], 1, 0
            ).astype(BF16)
    grads(1, 0, act1_s, dmix_s[:, 2 * D :])
    grads(1, 1, att_s, dproj_s[...])
    pair_start(1)
    pair_finish(1)
    total = add_all(prob_out, pgot, pmsg[me])
    pmine[...] = total
    start_all(prob_back)
    pg_s[me] = total
    total = add_all(small_out, sgot, smsg[me])
    ssend[...] = total
    srb[rep] = total

    def small_copy(k):
        return remote(ssend, srb.at[rep], s_small, 0, rep=lax.rem(rep + k, reps))

    smalls = srb.at[pl.ds(0, reps - 1)]
    small_all = remote(smalls, smalls, s_small, 0, rep=lax.rem(rep + 1, reps))

    for k in range(1, reps):
        small_copy(k).start()
    received(prob_back)

    for p in range(PAIRS):
        prob, scores, divisor, sharp, query_norm, key_norm = pair_attention(
            p, gram_s, sq_s, sharp_ref, low, eye
        )
        pg = pg_s[8 * p : 8 * p + 8].reshape(HEAD_DIM, 128)
        logit = prob * (pg - half_sum(prob * pg, low))
        bd2_s[p] = block_diag(logit * sharp / divisor, low)
        weighted = logit * scores
        d_qsq = -half_sum(weighted, low) / (2.0 * query_norm * query_norm)
        d_qsq = 2.0 * jnp.sum(jnp.where(eye, d_qsq, 0.0), 0, keepdims=True)
        d_ksq = -2.0 * jnp.sum(weighted, 0, keepdims=True) / (2.0 * key_norm * key_norm)
        qc = slice(128 * p, 128 * p + 128)
        kc = slice(D + 128 * p, D + 128 * p + 128)
        for i in range(0, TOK, 256):
            at = slice(i, i + 256)
            query, key = mixed_s[at, qc], mixed_s[at, kc]
            dmix_s[at, qc] = (dot(key, bd2_s[p], 1, 1) + d_qsq * query.astype(F32)).astype(BF16)
            dmix_s[at, kc] = (dot(query, bd2_s[p], 1, 0) + d_ksq * key.astype(F32)).astype(BF16)

    def inputs(i):
        at = ds(i * 256, 256)
        dact_s[at, :] = dot(dmix_s[at, :], w_ref[...], 1, 1)

    grads(0, 0, act1_s, dmix_s[:, :D])
    grads(0, 1, act1_s, dmix_s[:, D : 2 * D])
    pair_start(0)
    column_finish(1)
    pair_finish(0)
    loop(2, inputs)

    def input_rows(i):
        at = ds(i * 32, 32)
        normed, inverse = norm_parts(x_ref[at, :].astype(F32))
        lnb = norm_back(dact_s[at, :], gain1, normed, inverse)
        out_ref[at, :] = (dres_s[at, :] + lnb).astype(BF16)

    loop(TOK // 32, input_rows, each=4)
    column_finish(0)
    third_finish(1)
    small_all.wait_recv()
    total = srb[0]
    for k in range(1, reps):
        total = total + srb[k]
    sfin[...] = total
    small_ref[me] = total
    fifth = part_from(sfin, small_ref, s_fifth)
    start_all(fifth)
    third_finish(0)

    for copy in (gram_out, gram_back, sq_out, sq_back, prob_out, prob_back, small_out, third[0], third[1]):
        sent(copy)
    for src, halo, sems in (
        (up_row[0], up_halo, s_up),
        (act_edge.at[0], act_halo, s_act),
        (dh_edge.at[0], dh_halo, s_dh),
    ):
        halos_sent(src, halo, sems)
    small_all.wait_send()
    for half in range(2):
        for k in range(4):
            pair_copy(half, k).wait_send()
        for k in range(3):
            column_copy(half, k).wait_send()
    for copy in (fourth[1], fifth, fourth[0]):
        received(copy)
        sent(copy)


def finish(out_in, grads_ref, small_ref, out_ref, gq_ref, gp_ref, conv_ref, scale_ref):
    out_ref[...] = out_in[...]
    for j in range(32):
        rows, cols = chunk(j)
        gq_ref[rows, cols] = grads_ref[0, j].astype(F32)
        if cols.start < D:
            gq_ref[rows, 2 * D + cols.start : 2 * D + cols.stop] = grads_ref[1, j].astype(F32)
        else:
            gp_ref[rows, cols.start - D : cols.stop - D] = grads_ref[1, j].astype(F32)
    for at in range(80):
        v, b = at // 4, at % 4
        line = small_ref[at // 3, at % 3 : at % 3 + 1, :]
        lanes = slice(128 * b, 128 * b + 128)
        if v < 18:
            conv_ref[(v // 3) % 3, v % 3, v // 9 : v // 9 + 1, lanes] = line
        else:
            scale_ref[v - 18 : v - 17, lanes] = line


def call(body, name, outs, scratch, args, smem=0, collective=None, away=()):
    params = dict(vmem_limit_bytes=LIMIT)
    if collective is not None:
        params.update(collective_id=collective, has_side_effects=True)
    specs = [pl.BlockSpec(memory_space=pltpu.SMEM)] * smem
    specs += [
        pl.BlockSpec(memory_space=pl.ANY if at in away else VMEM) for at in range(smem, len(args))
    ]
    return pl.pallas_call(
        body,
        name=name,
        out_shape=[jax.ShapeDtypeStruct(s, t) for s, t in outs],
        in_specs=specs,
        out_specs=[pl.BlockSpec(memory_space=VMEM)] * len(outs),
        scratch_shapes=scratch,
        compiler_params=pltpu.CompilerParams(**params),
    )(*args)


def shards(n, x, up, gain1, w, sharp, wo, factors, gain2, kernels):
    x = x.reshape(TOK, D)
    up = up.reshape(TOK, D)
    gain1, gain2 = gain1.reshape(1, D), gain2.reshape(1, D)
    kernels = kernels.transpose(1, 2, 0, 3)
    row = VMEM((n, 8, 128), F32)
    edge = VMEM((2, WIDTH, D), BF16)
    wide, tall = VMEM((TOK, D), BF16), VMEM((TOK, D), F32)
    scratch = [pltpu.SMEM((HEADS,), F32), wide, VMEM((1, D), F32), VMEM((2, D), F32)]
    scratch += [VMEM((1, D), F32), VMEM((3, 3, 2, D), F32)]
    scratch += [wide, VMEM((D, 3 * D), BF16), wide, wide, VMEM((TOK, 3 * D), BF16)]
    scratch += [row, row, VMEM((8, 128), F32), row]
    scratch += [VMEM((n, 1, 128), F32), VMEM((n, 1, 128), F32), VMEM((1, 128), F32)]
    scratch += [VMEM((n, 1, 128), F32), VMEM((8, 128), F32), VMEM((18, D), F32)]
    scratch += [edge] * 5
    scratch += [VMEM((count, 272, D), F32) for count in (4, 4, 4, 2)]
    scratch += [tall, VMEM((PAIRS, 128, 128), BF16), VMEM((PAIRS, 128, 128), BF16)]
    scratch += [wide, tall, tall, VMEM((TOK, 128), F32), tall, VMEM((18, 8, D), F32)]
    scratch += [wide, tall, wide, VMEM((TOK, 3 * D), BF16)]
    scratch += [row, row, VMEM((8, 128), F32), row, row, row]
    scratch += [
        VMEM((2, 2, 4, 64, 1024), BF16),
        VMEM((2, 4, 64, 1024), BF16),
        VMEM((2, 3, 64, 1024), BF16),
        VMEM((2, 3, 64, 1024), BF16),
        VMEM((2, 64, 1024), F32),
        VMEM((2, n, 16, 128), BF16),
        VMEM((2, n, 16, 128), BF16),
        VMEM((2, 16, 128), BF16),
        VMEM((8, 8, 128), F32),
        VMEM((8, 128), F32),
        VMEM((8, 128), F32),
    ]
    for count in (9, 1, 1, 1, 1, 1, 1, 1, 2, 2, 2, 8, 6, 2, 2, 1, 1):
        scratch.append(pltpu.SemaphoreType.DMA((2, count)))
    out, grads, small = call(
        functools.partial(layer, n),
        "layer",
        [((TOK, D), BF16), ((2, n, 16, 128), BF16), ((n, 8, 128), F32)],
        scratch,
        (sharp, x, up, gain1, w, wo, factors, gain2, kernels),
        collective=0,
        away=range(9),
    )
    out, gq, gp, conv, scale = call(
        finish,
        "finish",
        [
            ((TOK, D), BF16),
            ((64, 3 * D), F32),
            ((64, D), F32),
            ((3, 3, 2, D), F32),
            ((2, D), F32),
        ],
        [],
        (out, grads, small),
    )
    return out.reshape(1, 2, WIDTH, D), gq, gp, conv.transpose(2, 0, 1, 3), scale


def solution(mesh):
    tokens = P("rep", "sp", None, None)
    in_specs = (tokens, tokens, P(), P(), P(), P(), P(), P(), P())
    out_specs = (tokens, P("rep", None), P("rep", None), P(), P())
    return jax.shard_map(
        functools.partial(shards, mesh.shape["sp"]),
        mesh=mesh,
        in_specs=in_specs,
        out_specs=out_specs,
        check_vma=False,
    )
```

```python
import functools

import jax
import jax.numpy as jnp
from jax import lax
from jax.experimental import pallas as pl
from jax.experimental.pallas import tpu as pltpu
from jax.sharding import PartitionSpec as P

D = 512
HEADS = 8
HEAD_DIM = 64
WIDTH = 256
EPS = 1e-06
F32 = jnp.float32
BF16 = jnp.bfloat16
TOK = 512
PAIRS = 4
VMEM = pltpu.VMEM
MESH_ID = pl.DeviceIdType.MESH
LIMIT = 60 * 1024 * 1024


def dot(a, b, ca, cb):
    return lax.dot_general(a, b, (((ca,), (cb,)), ((), ())), preferred_element_type=F32)


def ds(start, size, multiple=None):
    return pl.ds(pl.multiple_of(start, multiple or size), size)


def norm_parts(u):
    centre = jnp.mean(u, -1, keepdims=True)
    centred = u - centre
    inverse = lax.rsqrt(jnp.mean(centred * centred, -1, keepdims=True) + EPS)
    return centred * inverse, inverse


def norm_back(upstream, gain, normed, inverse):
    scaled = upstream * gain
    return inverse * (
        scaled
        - jnp.mean(scaled, -1, keepdims=True)
        - normed * jnp.mean(scaled * normed, -1, keepdims=True)
    )


def lane_low():
    return lax.broadcasted_iota(jnp.int32, (HEAD_DIM, 128), 1) < HEAD_DIM


def eye_pair():
    lane = lax.broadcasted_iota(jnp.int32, (HEAD_DIM, 128), 1)
    row = lax.broadcasted_iota(jnp.int32, (HEAD_DIM, 128), 0)
    return (lane == row) | (lane == row + HEAD_DIM)


def half_sum(v, low):
    left = jnp.sum(jnp.where(low, v, 0.0), -1, keepdims=True)
    right = jnp.sum(jnp.where(low, 0.0, v), -1, keepdims=True)
    return jnp.where(low, left, right)


def half_max(v, low):
    left = jnp.max(jnp.where(low, v, -jnp.inf), -1, keepdims=True)
    right = jnp.max(jnp.where(low, -jnp.inf, v), -1, keepdims=True)
    return jnp.where(low, left, right)


def pack_pair(full, low):
    return jnp.where(low, full[:HEAD_DIM], full[HEAD_DIM:])


def block_diag(packed, low):
    return jnp.concatenate(
        [jnp.where(low, packed, 0.0), jnp.where(low, 0.0, packed)], axis=0
    ).astype(BF16)


def pair_attention(p, gram_ref, sq_ref, sharp_ref, low, eye):
    gram = gram_ref[8 * p : 8 * p + 8].reshape(HEAD_DIM, 128)
    query_sq = half_sum(jnp.where(eye, sq_ref[p : p + 1, :], 0.0), low)
    query_norm = jnp.sqrt(query_sq + EPS)
    key_norm = jnp.sqrt(sq_ref[PAIRS + p : PAIRS + p + 1, :] + EPS)
    divisor = query_norm * key_norm
    sharp = jnp.where(low, sharp_ref[2 * p], sharp_ref[2 * p + 1])
    scores = sharp * gram / divisor
    exponent = jnp.exp(scores - half_max(scores, low))
    prob = exponent / half_sum(exponent, low)
    return prob, scores, divisor, sharp, query_norm, key_norm


def remote(src, dst, sems, at, **axes):
    return pltpu.make_async_remote_copy(
        src_ref=src,
        dst_ref=dst,
        send_sem=sems.at[0, at],
        recv_sem=sems.at[1, at],
        device_id=axes,
        device_id_type=MESH_ID,
    )


def loop(count, step, first=0, each=1):
    def go(i, _):
        for u in range(each):
            step(i * each + u)
        return 0

    lax.fori_loop(first, count // each, go, 0)


def fold(v):
    return v.reshape(-1, 8, v.shape[-1]).sum(0)


def chunk(j):
    return slice(16 * (j // 8), 16 * (j // 8) + 16), slice(128 * (j % 8), 128 * (j % 8) + 128)


def layer(
    n,
    sharp_hbm,
    x_hbm,
    up_hbm,
    gain1_hbm,
    w_hbm,
    wo_hbm,
    factor_hbm,
    gain2_hbm,
    kern4_hbm,
    out_ref,
    grads_ref,
    small_ref,
    sharp_ref,
    x_ref,
    gain1_ref,
    factor_ref,
    gain2_ref,
    kern4_ref,
    up_ref,
    w_ref,
    wo_ref,
    act1_s,
    mixed_s,
    gmsg,
    ggot,
    gmine,
    gram_s,
    gsq,
    gsqgot,
    gsqmine,
    sq_all,
    sq_s,
    kern_ref,
    up_halo,
    act_halo,
    dh_halo,
    act_edge,
    dh_edge,
    act_s,
    up_s,
    dh_s,
    hid_s,
    dhid_s,
    bd_s,
    bd2_s,
    att_s,
    proj_s,
    normed_s,
    inv_s,
    dact_s,
    acc_s,
    dproj_s,
    dres_s,
    datt_s,
    dmix_s,
    pmsg,
    pgot,
    pmine,
    pg_s,
    smsg,
    sgot,
    gl,
    rb1,
    sb2,
    rb2,
    acc2,
    sb3,
    rb3,
    fin,
    srb,
    ssend,
    sfin,
    s_load,
    s_g1,
    s_g2,
    s_q1,
    s_q2,
    s_p1,
    s_p2,
    s_s1,
    s_up,
    s_act,
    s_dh,
    s_pair,
    s_col,
    s_third,
    s_fourth,
    s_small,
    s_fifth,
):
    me, rep = lax.axis_index("sp"), lax.axis_index("rep")
    reps = 8
    moves = (
        (x_hbm, x_ref),
        (gain1_hbm, gain1_ref),
        (w_hbm, w_ref),
        (up_hbm, up_ref),
        (wo_hbm, wo_ref),
        (sharp_hbm, sharp_ref),
        (factor_hbm, factor_ref),
        (gain2_hbm, gain2_ref),
        (kern4_hbm, kern4_ref),
    )
    loads = [
        pltpu.make_async_copy(src, dst, s_load.at[0, at]) for at, (src, dst) in enumerate(moves)
    ]
    y, core = rep // 2, lax.rem(rep, 2)
    barrier = pltpu.get_barrier_semaphore()
    loads[0].start()
    loads[1].start()

    def greet(k):
        pl.semaphore_signal(
            barrier, inc=1, device_id={"sp": lax.rem(me + k, n)}, device_id_type=MESH_ID
        )

    loop(n, greet, 1)
    for k in range(1, reps):
        pl.semaphore_signal(
            barrier, inc=1, device_id={"rep": lax.rem(rep + k, reps)}, device_id_type=MESH_ID
        )
    for load in loads[2:]:
        load.start()
    low, eye = lane_low(), eye_pair()

    half_row = WIDTH // 2

    def to_above(src, halo, sems, half):
        at = pl.ds(half * half_row, half_row)
        return remote(src.at[at], halo.at[1, at], sems, half, sp=me - 1)

    def to_below(src, halo, sems, half):
        at = pl.ds(half * half_row, half_row)
        return remote(src.at[at], halo.at[0, at], sems, 2 + half, sp=me + 1)

    def send_above(src, halo, sems, halves=(0, 1)):
        @pl.when(me > 0)
        def _():
            for half in halves:
                to_above(src, halo, sems, half).start()

    def send_below(src, halo, sems, halves=(0, 1)):
        @pl.when(me < n - 1)
        def _():
            for half in halves:
                to_below(src, halo, sems, half).start()

    def halos_in(src, halo, sems):
        @pl.when(me > 0)
        def _():
            for half in range(2):
                to_below(src, halo, sems, half).wait_recv()

        @pl.when(me == 0)
        def _():
            halo[0] = jnp.zeros((WIDTH, D), BF16)

        @pl.when(me < n - 1)
        def _():
            for half in range(2):
                to_above(src, halo, sems, half).wait_recv()

        @pl.when(me == n - 1)
        def _():
            halo[1] = jnp.zeros((WIDTH, D), BF16)

    def halos_sent(src, halo, sems):
        @pl.when(me > 0)
        def _():
            for half in range(2):
                to_above(src, halo, sems, half).wait_send()

        @pl.when(me < n - 1)
        def _():
            for half in range(2):
                to_below(src, halo, sems, half).wait_send()

    def spread(halo, target):
        def rows(i):
            side, c = i // 4, lax.rem(i, 4)
            target[3 * side, ds(8 + c * 64, 64, 8), :] = halo[side, ds(c * 64, 64), :].astype(F32)

        loop(8, rows)

    class Group:
        def __init__(self, copy, sent, got, sems, at=0):
            self.copy = copy
            near = {"sp": lax.rem(me + 1, n)}
            self.whole = remote(sent, got, sems, at, **near)

    def part_to(msg, got, sems, at=0):
        def copy(k):
            j = lax.rem(me + k, n)
            return remote(msg.at[j], got.at[k], sems, at, sp=j)

        rest = pl.ds(1, n - 1)
        return Group(copy, msg.at[rest], got.at[rest], sems, at)

    def part_from(mine, total, sems, at=0):
        def copy(k):
            return remote(mine, total.at[me], sems, at, sp=lax.rem(me + k, n))

        rest = pl.ds(0, n - 1)
        return Group(copy, total.at[rest], total.at[rest], sems, at)

    def start_all(*groups):
        def start(t):
            k = n // 2 + (t // 2) * (1 - 2 * lax.rem(t, 2))
            for group in groups:
                group.copy(k).start()

        loop(n, start, 1)

    def add_all(group, got, own):
        received(group)
        for k in range(1, n):
            own = own + got[k].astype(F32)
        return own

    def received(group):
        group.whole.wait_recv()

    def sent(group):
        group.whole.wait_send()

    loads[0].wait()
    loads[1].wait()
    gain1 = gain1_ref[...]

    def norm_one(i):
        at = ds(i * 32, 32)
        normed, _ = norm_parts(x_ref[at, :].astype(F32))
        act1_s[at, :] = (normed * gain1).astype(BF16)

    loop(TOK // 32, norm_one, each=4)
    loads[2].wait()

    def mix(i):
        at = ds(i * 256, 256)
        mixed_s[at, :] = dot(act1_s[at, :], w_ref[...], 1, 0).astype(BF16)

    loop(2, mix)
    lines = []
    for p in range(2 * PAIRS):
        sq = jnp.zeros((8, 128), F32)
        for i in range(0, TOK, 64):
            part = mixed_s[i : i + 64, 128 * p : 128 * p + 128].astype(F32)
            sq = sq + fold(part * part)
        lines.append(sq.sum(0, keepdims=True))
    sq = jnp.concatenate(lines, axis=0)
    for p in range(PAIRS):
        query = mixed_s[:, 128 * p : 128 * p + 128]
        key = mixed_s[:, D + 128 * p : D + 128 * p + 128]
        packed = pack_pair(dot(query, key, 0, 0), low)
        for b in range(8):
            gmsg[8 * p + b] = packed[8 * b : 8 * b + 8]
    quarter = lax.broadcasted_iota(jnp.int32, (1, 128), 1) >> 5
    for j in range(n):
        gsq[j] = jnp.where(quarter == j % 4, sq[j // 4 : j // 4 + 1], 0.0)
    pl.semaphore_wait(barrier, n - 1 + reps - 1)
    gram_out, gram_back = part_to(gmsg, ggot, s_g1), part_from(gmine, gram_s, s_g2)
    sq_out, sq_back = part_to(gsq, gsqgot, s_q1), part_from(gsqmine, sq_all, s_q2)
    start_all(gram_out, sq_out)
    up_row = [up_ref.at[pl.ds(0, WIDTH)], up_ref.at[pl.ds(WIDTH, WIDTH)]]

    for load in loads[3:]:
        load.wait()
    gain2 = gain2_ref[...]
    factor0, factor1 = factor_ref[0:1, :], factor_ref[1:2, :]
    for at in range(18):
        kern_ref[at : at + 1, :] = kern4_ref[(at // 3) % 3, at % 3, at // 9 : at // 9 + 1, :]
    for ref, count in ((act_s, 4), (up_s, 4), (dh_s, 4), (hid_s, 2)):
        for r in range(count):
            ref[r, 0:8, :] = jnp.zeros((8, D), F32)
            ref[r, 264:272, :] = jnp.zeros((8, D), F32)
    acc_s[...] = jnp.zeros_like(acc_s)

    def upstream_rows(i):
        row, c = i // 4, lax.rem(i, 4)
        up_s[row + 1, ds(8 + c * 64, 64, 8), :] = up_ref[ds(i * 64, 64), :].astype(F32)

    loop(8, upstream_rows)
    total = add_all(gram_out, ggot, gmsg[me])
    gmine[...] = total
    gram_s[me] = total
    total = add_all(sq_out, gsqgot, gsq[me])
    gsqmine[...] = total
    sq_all[me] = total
    start_all(gram_back, sq_back)
    send_above(up_row[0], up_halo, s_up)
    send_below(up_row[1], up_halo, s_up)
    received(gram_back)
    received(sq_back)
    for p in range(2 * PAIRS):
        sq_s[p : p + 1, :] = sq_all[4 * p] + sq_all[4 * p + 1] + sq_all[4 * p + 2] + sq_all[4 * p + 3]

    for p in range(PAIRS):
        prob = pair_attention(p, gram_s, sq_s, sharp_ref, low, eye)[0]
        bd_s[p] = block_diag(prob, low)
    for row in range(2):
        at_row = slice(row * WIDTH, row * WIDTH + WIDTH)
        for p in range(PAIRS):
            cols = slice(128 * p, 128 * p + 128)
            value = mixed_s[at_row, 2 * D + 128 * p : 2 * D + 128 * p + 128]
            att_s[at_row, cols] = dot(value, bd_s[p], 1, 1).astype(BF16)
        proj_s[at_row, :] = dot(att_s[at_row, :], wo_ref[...], 1, 0)

    for half, row in ((0, 0), (0, 1), (1, 0), (1, 1)):

        def norm_two(i, half=half, row=row):
            c = 4 * half + i
            at = ds(row * WIDTH + c * 32, 32)
            u = x_ref[at, :].astype(F32) + factor0 * proj_s[at, :]
            normed, inverse = norm_parts(u.astype(BF16).astype(F32))
            act = (normed * gain2).astype(BF16)
            act_edge[row, ds(c * 32, 32), :] = act
            act_s[row + 1, ds(8 + c * 32, 32, 8), :] = act.astype(F32)
            normed_s[at, :] = normed
            inv_s[at, :] = jnp.broadcast_to(inverse, (32, 128))

        loop(4, norm_two, each=4)
        if row == 0:
            send_above(act_edge.at[0], act_halo, s_act, (half,))
        else:
            send_below(act_edge.at[1], act_halo, s_act, (half,))

    def taps(which, lanes, i, j):
        at = 9 * which + 3 * i + j
        return kern_ref[at : at + 1, lanes]

    def place(idx):
        return ds((idx // 4) * 128, 128), lax.rem(idx, 4)

    def forth(sums):
        return pltpu.roll(sums[0], 1, 0)[8:72] + sums[1][8:72] + pltpu.roll(sums[2], 79, 0)[8:72]

    def back(sums):
        return pltpu.roll(sums[0], 79, 0)[8:72] + sums[1][8:72] + pltpu.roll(sums[2], 1, 0)[8:72]

    halos_in(up_row[0], up_halo, s_up)
    spread(up_halo, up_s)

    def hidden_grads(idx):
        r = idx // 16
        lanes, c = place(lax.rem(idx, 16))
        win = ds(c * 64, 80, 8)
        near = [up_s[r + 2 - i, win, lanes] for i in range(3)]
        scale = factor_ref[1:2, lanes]
        sums = [sum((taps(1, lanes, i, j) * scale) * near[i] for i in range(3)) for j in range(3)]
        dhid_s[ds(r * WIDTH + c * 64, 64), lanes] = back(sums)

    loop(32, hidden_grads)

    def own_part(target, source, rows, join):
        for r in range(2):

            def go(idx, r=r):
                lanes, c = place(idx)
                win = ds(c * 64, 80, 8)
                near = {i: source[rows(r, i), win, lanes] for i in range(3) if rows(r, i) in (1, 2)}
                target[ds(r * WIDTH + c * 64, 64), lanes] = join(
                    [sum(taps(0, lanes, i, j) * near[i] for i in near) for j in range(3)]
                )

            loop(16, go)

    def halo_part(source, row, i, win, lanes, join):
        near = source[row, win, lanes]
        return join([taps(0, lanes, i, j) * near for j in range(3)])

    own_part(dact_s, act_s, lambda r, i: r + i, forth)
    halos_in(act_edge.at[0], act_halo, s_act)
    spread(act_halo, act_s)
    for half, r in ((0, 0), (0, 1), (1, 0), (1, 1)):

        def hidden_row(idx, half=half, r=r):
            lanes, c = ds((idx // 2) * 128, 128), 2 * half + lax.rem(idx, 2)
            win, mid = ds(c * 64, 80, 8), ds(8 + c * 64, 64, 8)
            h = dact_s[ds(r * WIDTH + c * 64, 64), lanes] + halo_part(
                act_s, 3 * r, 2 * r, win, lanes, forth
            )
            cumul = 0.5 * (1.0 + lax.erf(h * 0.7071067811865476))
            density = jnp.exp(-0.5 * h * h) * 0.3989422804014327
            hid_s[r, mid, lanes] = (h * cumul).astype(BF16).astype(F32)
            d_h = dhid_s[ds(r * WIDTH + c * 64, 64), lanes] * (cumul + h * density)
            dh_s[r + 1, mid, lanes] = d_h
            dh_edge[r, ds(c * 64, 64), lanes] = d_h.astype(BF16)

        loop(8, hidden_row)
        if r == 0:
            send_above(dh_edge.at[0], dh_halo, s_dh, (half,))
        else:
            send_below(dh_edge.at[1], dh_halo, s_dh, (half,))

    def kernel_grads(idx):
        r = idx // 16
        lanes, c = place(lax.rem(idx, 16))
        win, mid = ds(c * 64, 80, 8), ds(8 + c * 64, 64, 8)
        own = dh_s[r + 1, win, lanes]
        moved = [pltpu.roll(own, 79, 0)[8:72], own[8:72], pltpu.roll(own, 1, 0)[8:72]]
        for i in range(3):
            act = act_s[r + i, mid, lanes]
            for j in range(3):
                acc_s[3 * i + j, :, lanes] += fold(moved[j] * act)
        own = hid_s[r, win, lanes]
        moved = [pltpu.roll(own, 1, 0)[8:72], own[8:72], pltpu.roll(own, 79, 0)[8:72]]
        for i in range(3):
            up = up_s[r + 2 - i, mid, lanes]
            for j in range(3):
                acc_s[9 + 3 * i + j, :, lanes] += fold(moved[j] * up)

    loop(32, kernel_grads)
    own_part(dact_s, dh_s, lambda r, i: r + 2 - i, back)
    halos_in(dh_edge.at[0], dh_halo, s_dh)
    spread(dh_halo, dh_s)

    for r in range(2):

        def act_grads(idx, r=r):
            lanes, c = place(idx)
            win, at = ds(c * 64, 80, 8), ds(r * WIDTH + c * 64, 64)
            dact_s[at, lanes] = dact_s[at, lanes] + halo_part(
                dh_s, 3 * r, 2 - 2 * r, win, lanes, back
            )

        loop(16, act_grads)

    def residual_rows(step, scale):
        for u in range(4):
            i = 4 * step + u
            row, c = i // 8, lax.rem(i, 8)
            at = ds(i * 32, 32)
            lnb = norm_back(dact_s[at, :], gain2, normed_s[at, :], inv_s[at, 0:1])
            d_res = up_s[row + 1, ds(8 + c * 32, 32, 8), :] + lnb
            dres_s[at, :] = d_res
            dproj_s[at, :] = (factor0 * d_res).astype(BF16)
            scale = scale + fold(proj_s[at, :] * d_res)
        return scale

    scale_one = lax.fori_loop(0, TOK // 128, residual_rows, jnp.zeros((8, D), F32))

    def attended_rows(i):
        at = ds(i * 256, 256)
        datt_s[at, :] = dot(dproj_s[at, :], wo_ref[...], 1, 1).astype(BF16)

    loop(2, attended_rows)
    for p in range(PAIRS):
        cols = slice(128 * p, 128 * p + 128)
        value = mixed_s[:, 2 * D + 128 * p : 2 * D + 128 * p + 128]
        packed = pack_pair(dot(datt_s[:, cols], value, 0, 0), low)
        for b in range(8):
            pmsg[8 * p + b] = packed[8 * b : 8 * b + 8]
    prob_out, prob_back = part_to(pmsg, pgot, s_p1), part_from(pmine, pg_s, s_p2)
    start_all(prob_out)
    lines = [acc_s[m].sum(0, keepdims=True) for m in range(18)]
    scale_two = sum(lines[9 + m] * kern_ref[9 + m : 10 + m, :] for m in range(9))
    lines = lines[:9] + [line * factor1 for line in lines[9:]]
    lines += [scale_one.sum(0, keepdims=True), scale_two]
    smsg[...] = jnp.zeros_like(smsg)
    for at in range(80):
        v, b = at // 4, at % 4
        smsg[at // 3, at % 3 : at % 3 + 1, :] = lines[v][:, 128 * b : 128 * b + 128]
    small_out = part_to(smsg, sgot, s_s1)
    start_all(small_out)

    def grads(half, block, left, right):
        for side in range(2):
            g = dot(left[:, 256 * side : 256 * side + 256], right, 0, 0).astype(BF16)
            for r in range(4):
                at = 4 * side + r
                gl[half, at % 2, at // 2, :, 512 * block : 512 * block + 512] = g[
                    64 * r : 64 * r + 64
                ]

    def pair_copy(half, k):
        there = lax.rem(y + 1 + k, 4)
        return remote(
            gl.at[half, 1 - core, there],
            rb1.at[half, k],
            s_pair,
            4 * half + k,
            rep=2 * y + 1 - core,
        )

    def column_copy(half, k):
        there = lax.rem(y + 1 + k, 4)
        return remote(
            sb2.at[half, k], rb2.at[half, k], s_col, 3 * half + k, rep=2 * there + core
        )

    def pair_start(half):
        for k in range(4):
            pair_copy(half, k).start()

    def pair_finish(half):
        for k in range(3):
            there = lax.rem(y + 1 + k, 4)
            pair_copy(half, k).wait_recv()

            def add(i, k=k, there=there):
                at = ds(i * 16, 16)
                sb2[half, k, at, :] = (
                    gl[half, core, there, at, :].astype(F32) + rb1[half, k, at, :].astype(F32)
                ).astype(BF16)

            loop(4, add)
            column_copy(half, k).start()
        pair_copy(half, 3).wait_recv()

        def own(i):
            at = ds(i * 16, 16)
            acc2[half, at, :] = gl[half, core, y, at, :].astype(F32) + rb1[half, 3, at, :].astype(
                F32
            )

        loop(4, own)

    third = [part_to(sb3.at[half], rb3.at[half], s_third, half) for half in range(2)]
    fourth = [
        part_from(fin.at[half], grads_ref.at[half], s_fourth, half) for half in range(2)
    ]

    def column_finish(half):
        for k in range(3):
            column_copy(half, k).wait_recv()
        for j in range(n):
            rows, cols = chunk(j)
            total = acc2[half, rows, cols]
            for k in range(3):
                total = total + rb2[half, k, rows, cols].astype(F32)
            sb3[half, j] = total.astype(BF16)
        start_all(third[half])

    def third_finish(half):
        total = add_all(third[half], rb3.at[half], sb3[half, me].astype(F32)).astype(BF16)
        fin[half] = total
        grads_ref[half, me] = total
        start_all(fourth[half])

    for p in range(PAIRS):
        cols = slice(128 * p, 128 * p + 128)
        for i in range(0, TOK, 256):
            dmix_s[i : i + 256, 2 * D + 128 * p : 2 * D + 128 * p + 128] = dot(
                datt_s[i : i + 256, cols], bd_s[p], 1, 0
            ).astype(BF16)
    grads(1, 0, act1_s, dmix_s[:, 2 * D :])
    grads(1, 1, att_s, dproj_s[...])
    pair_start(1)
    pair_finish(1)
    total = add_all(prob_out, pgot, pmsg[me])
    pmine[...] = total
    start_all(prob_back)
    pg_s[me] = total
    total = add_all(small_out, sgot, smsg[me])
    ssend[...] = total
    srb[rep] = total

    def small_copy(k):
        return remote(ssend, srb.at[rep], s_small, 0, rep=lax.rem(rep + k, reps))

    smalls = srb.at[pl.ds(0, reps - 1)]
    small_all = remote(smalls, smalls, s_small, 0, rep=lax.rem(rep + 1, reps))

    for k in range(1, reps):
        small_copy(k).start()
    received(prob_back)

    for p in range(PAIRS):
        prob, scores, divisor, sharp, query_norm, key_norm = pair_attention(
            p, gram_s, sq_s, sharp_ref, low, eye
        )
        pg = pg_s[8 * p : 8 * p + 8].reshape(HEAD_DIM, 128)
        logit = prob * (pg - half_sum(prob * pg, low))
        bd2_s[p] = block_diag(logit * sharp / divisor, low)
        weighted = logit * scores
        d_qsq = -half_sum(weighted, low) / (2.0 * query_norm * query_norm)
        d_qsq = 2.0 * jnp.sum(jnp.where(eye, d_qsq, 0.0), 0, keepdims=True)
        d_ksq = -2.0 * jnp.sum(weighted, 0, keepdims=True) / (2.0 * key_norm * key_norm)
        qc = slice(128 * p, 128 * p + 128)
        kc = slice(D + 128 * p, D + 128 * p + 128)
        for i in range(0, TOK, 256):
            at = slice(i, i + 256)
            query, key = mixed_s[at, qc], mixed_s[at, kc]
            dmix_s[at, qc] = (dot(key, bd2_s[p], 1, 1) + d_qsq * query.astype(F32)).astype(BF16)
            dmix_s[at, kc] = (dot(query, bd2_s[p], 1, 0) + d_ksq * key.astype(F32)).astype(BF16)

    def inputs(i):
        at = ds(i * 256, 256)
        dact_s[at, :] = dot(dmix_s[at, :], w_ref[...], 1, 1)

    grads(0, 0, act1_s, dmix_s[:, :D])
    grads(0, 1, act1_s, dmix_s[:, D : 2 * D])
    pair_start(0)
    column_finish(1)
    pair_finish(0)
    loop(2, inputs)

    def input_rows(i):
        at = ds(i * 32, 32)
        normed, inverse = norm_parts(x_ref[at, :].astype(F32))
        lnb = norm_back(dact_s[at, :], gain1, normed, inverse)
        out_ref[at, :] = (dres_s[at, :] + lnb).astype(BF16)

    loop(TOK // 32, input_rows, each=4)
    column_finish(0)
    third_finish(1)
    small_all.wait_recv()
    total = srb[0]
    for k in range(1, reps):
        total = total + srb[k]
    sfin[...] = total
    small_ref[me] = total
    fifth = part_from(sfin, small_ref, s_fifth)
    start_all(fifth)
    third_finish(0)

    for copy in (gram_out, gram_back, sq_out, sq_back, prob_out, prob_back, small_out, third[0], third[1]):
        sent(copy)
    for src, halo, sems in (
        (up_row[0], up_halo, s_up),
        (act_edge.at[0], act_halo, s_act),
        (dh_edge.at[0], dh_halo, s_dh),
    ):
        halos_sent(src, halo, sems)
    small_all.wait_send()
    for half in range(2):
        for k in range(4):
            pair_copy(half, k).wait_send()
        for k in range(3):
            column_copy(half, k).wait_send()
    for copy in (fourth[1], fifth, fourth[0]):
        received(copy)
        sent(copy)


def finish(out_in, grads_ref, small_ref, out_ref, gq_ref, gp_ref, conv_ref, scale_ref):
    out_ref[...] = out_in[...]
    for j in range(32):
        rows, cols = chunk(j)
        gq_ref[rows, cols] = grads_ref[0, j].astype(F32)
        if cols.start < D:
            gq_ref[rows, 2 * D + cols.start : 2 * D + cols.stop] = grads_ref[1, j].astype(F32)
        else:
            gp_ref[rows, cols.start - D : cols.stop - D] = grads_ref[1, j].astype(F32)
    for at in range(80):
        v, b = at // 4, at % 4
        line = small_ref[at // 3, at % 3 : at % 3 + 1, :]
        lanes = slice(128 * b, 128 * b + 128)
        if v < 18:
            conv_ref[(v // 3) % 3, v % 3, v // 9 : v // 9 + 1, lanes] = line
        else:
            scale_ref[v - 18 : v - 17, lanes] = line


def call(body, name, outs, scratch, args, smem=0, collective=None, away=()):
    params = dict(vmem_limit_bytes=LIMIT)
    if collective is not None:
        params.update(collective_id=collective, has_side_effects=True)
    specs = [pl.BlockSpec(memory_space=pltpu.SMEM)] * smem
    specs += [
        pl.BlockSpec(memory_space=pl.ANY if at in away else VMEM) for at in range(smem, len(args))
    ]
    return pl.pallas_call(
        body,
        name=name,
        out_shape=[jax.ShapeDtypeStruct(s, t) for s, t in outs],
        in_specs=specs,
        out_specs=[pl.BlockSpec(memory_space=VMEM)] * len(outs),
        scratch_shapes=scratch,
        compiler_params=pltpu.CompilerParams(**params),
    )(*args)


def shards(n, x, up, gain1, w, sharp, wo, factors, gain2, kernels):
    x = x.reshape(TOK, D)
    up = up.reshape(TOK, D)
    gain1, gain2 = gain1.reshape(1, D), gain2.reshape(1, D)
    kernels = kernels.transpose(1, 2, 0, 3)
    row = VMEM((n, 8, 128), F32)
    edge = VMEM((2, WIDTH, D), BF16)
    wide, tall = VMEM((TOK, D), BF16), VMEM((TOK, D), F32)
    scratch = [pltpu.SMEM((HEADS,), F32), wide, VMEM((1, D), F32), VMEM((2, D), F32)]
    scratch += [VMEM((1, D), F32), VMEM((3, 3, 2, D), F32)]
    scratch += [wide, VMEM((D, 3 * D), BF16), wide, wide, VMEM((TOK, 3 * D), BF16)]
    scratch += [row, row, VMEM((8, 128), F32), row]
    scratch += [VMEM((n, 1, 128), F32), VMEM((n, 1, 128), F32), VMEM((1, 128), F32)]
    scratch += [VMEM((n, 1, 128), F32), VMEM((8, 128), F32), VMEM((18, D), F32)]
    scratch += [edge] * 5
    scratch += [VMEM((count, 272, D), F32) for count in (4, 4, 4, 2)]
    scratch += [tall, VMEM((PAIRS, 128, 128), BF16), VMEM((PAIRS, 128, 128), BF16)]
    scratch += [wide, tall, tall, VMEM((TOK, 128), F32), tall, VMEM((18, 8, D), F32)]
    scratch += [wide, tall, wide, VMEM((TOK, 3 * D), BF16)]
    scratch += [row, row, VMEM((8, 128), F32), row, row, row]
    scratch += [
        VMEM((2, 2, 4, 64, 1024), BF16),
        VMEM((2, 4, 64, 1024), BF16),
        VMEM((2, 3, 64, 1024), BF16),
        VMEM((2, 3, 64, 1024), BF16),
        VMEM((2, 64, 1024), F32),
        VMEM((2, n, 16, 128), BF16),
        VMEM((2, n, 16, 128), BF16),
        VMEM((2, 16, 128), BF16),
        VMEM((8, 8, 128), F32),
        VMEM((8, 128), F32),
        VMEM((8, 128), F32),
    ]
    for count in (9, 1, 1, 1, 1, 1, 1, 1, 4, 4, 4, 8, 6, 2, 2, 1, 1):
        scratch.append(pltpu.SemaphoreType.DMA((2, count)))
    out, grads, small = call(
        functools.partial(layer, n),
        "layer",
        [((TOK, D), BF16), ((2, n, 16, 128), BF16), ((n, 8, 128), F32)],
        scratch,
        (sharp, x, up, gain1, w, wo, factors, gain2, kernels),
        collective=0,
        away=range(9),
    )
    out, gq, gp, conv, scale = call(
        finish,
        "finish",
        [
            ((TOK, D), BF16),
            ((64, 3 * D), F32),
            ((64, D), F32),
            ((3, 3, 2, D), F32),
            ((2, D), F32),
        ],
        [],
        (out, grads, small),
    )
    return out.reshape(1, 2, WIDTH, D), gq, gp, conv.transpose(2, 0, 1, 3), scale


def solution(mesh):
    tokens = P("rep", "sp", None, None)
    in_specs = (tokens, tokens, P(), P(), P(), P(), P(), P(), P())
    out_specs = (tokens, P("rep", None), P("rep", None), P(), P())
    return jax.shard_map(
        functools.partial(shards, mesh.shape["sp"]),
        mesh=mesh,
        in_specs=in_specs,
        out_specs=out_specs,
        check_vma=False,
    )
```
